32 devices in a mesh: cfg: 2 (over y), tm: 4 (over z), space: 2 (over x), spin: 2 (over core).
Axes of the slice: x: 2, y: 2, z: 4, core: 2. Of those that a mesh axis runs over, the one named last changes fastest.
Arguments:
- eigenvectors: bfloat16 [16, 2048, 3, 128], P(('cfg', 'tm'), ('space', 'spin')), parts along dimension 0, may hold values from -1.25 to 1.25
- momenta: int32 [8, 3], replicated, may hold values from -2 to 2, as said below
- time_pairs: int32 [32, 2], P(('cfg', 'tm')), parts along dimension 0, may hold values from 0 to 7
- slot_map: int32 [8], replicated, may hold values from 0 to 7, each once
- perambulators: bfloat16 [32, 64, 2048], P(('cfg', 'tm')), parts along dimension 0, may hold values from -0.046875 to 0.046875
Outputs:
- meson_loops: bfloat16 [32, 8, 64, 16, 128], P(('cfg', 'tm'), None, ('space', 'spin')), parts along dimension 0
The draws below stay inside these ranges and needn't reach their ends.
There are 2 independent parts, one for each index of `cfg`. The reference program is written for one: setup_inputs(seed, part) draws one part's arguments, and reference() takes and returns one part's arrays. A program takes and returns all parts, laid end to end along the dimension named above; an argument that names none is the same for every part. Nothing has to cross between parts.
Inputs may be any that keep to these rules, and one draw needn't show every extreme that they name: `momenta`: every momentum row has a component that is not zero. slot_map is a permutation of the 8 stored rows.
All inputs are finite; a program needn't handle non-finite values.
Results may differ from the reference program's by a relative error of at most 0.0074.
Values may be sent and summed in bfloat16 or wider, within the bound.
No kernel may reach another device: no remote copies, remote signals or barrier semaphores. Data moves between devices by JAX's collectives and lax.ppermute only.
A program may use at most 64 MiB of HBM per device.

```python
import jax
import jax.numpy as jnp
from jax import lax

NEV = 64
NMOM = 8
LAT = 32
SITES = 2048
NT = 8
PAIRS = 16


def draw_momenta(key, part):
    values = jax.random.randint(jax.random.fold_in(key, 11), (NMOM, 3), -2, 3).astype(jnp.int32)
    silent = jnp.all(values == 0, axis=1)
    bumped = jnp.where(silent, 1, 0).astype(jnp.int32)
    return values.at[:, 0].add(bumped)


def plant(array, own_key, low, top_value):
    index_at = [jax.random.randint(jax.random.fold_in(own_key, axis), (), 0, length) for axis, length in enumerate(array.shape)]
    widest = array.shape.index(max(array.shape))
    neighbour = index_at[:widest] + [(index_at[widest] + 1) % array.shape[widest]] + index_at[widest + 1:]
    return array.at[tuple(index_at)].set(low).at[tuple(neighbour)].set(top_value)


def levels(own_key, shape, shards, smallest, largest):
    factor_of = 1.0
    for position, blocks in shards:
        steps = jax.random.uniform(jax.random.fold_in(jax.random.fold_in(own_key, 6), position), (blocks,), jnp.float32, smallest / len(shards), largest / len(shards))
        factor_of = factor_of * jnp.repeat(jnp.exp(steps), shape[position] // blocks).reshape((-1,) + (1,) * (len(shape) - 1 - position))
    return factor_of


def normal_values(rng, extent, deviation, most, cuts=(), held_as=jnp.bfloat16):
    gain = levels(rng, extent, cuts, -0.22, 0.18) if cuts else 1.0
    array = jax.random.normal(rng, extent, jnp.float32) * deviation * gain
    return jnp.minimum(jnp.maximum(array, -most), most).astype(held_as)


def setup_inputs(seed: int = 0, part: int = 0) -> dict:
    key_list = jax.random.split(jax.random.key(seed), 6)
    part_splits = jax.random.split(jax.random.fold_in(key_list[5], part), 6)
    eigenvectors = normal_values(part_splits[0], (NT, SITES, 3, 2 * NEV), (1.0 / (12 * SITES) ** 0.25), 1.25, ((0, 4), (1, 4)))
    momenta = draw_momenta(jax.random.fold_in(key_list[5], 71), part)
    time_pairs = plant(jax.random.randint(part_splits[2], (PAIRS, 2), 0, NT), jax.random.fold_in(part_splits[2], 1), 0, NT - 1).astype(jnp.int32)
    slot_map = jax.random.permutation(key_list[3], NT).astype(jnp.int32)
    perambulators = normal_values(part_splits[4], (PAIRS, NEV, 32 * NEV), (4 * NEV * NEV) ** -0.5, 0.046875, ((0, 4),))
    return dict(eigenvectors=eigenvectors, momenta=momenta, time_pairs=time_pairs, slot_map=slot_map, perambulators=perambulators)


TURN = 6.283185307179586


def elemental(time_slab, momenta, first_site):
    site_count = time_slab.shape[0]
    vectors = time_slab.shape[2] // 2
    site_ids = first_site + lax.iota(jnp.int32, site_count)
    coord_x = site_ids % LAT
    coord_y = (site_ids // LAT) % LAT
    coord_z = site_ids // (LAT * LAT)
    real_part = time_slab[:, :, :vectors].astype(jnp.float32)
    imag_part = time_slab[:, :, vectors:].astype(jnp.float32)
    conj_left = time_slab.reshape(site_count * 6, vectors)
    results = []
    for momentum_row in range(momenta.shape[0]):
        wavenum = jnp.mod(momenta[momentum_row, 0] * coord_x + momenta[momentum_row, 1] * coord_y + momenta[momentum_row, 2] * coord_z, LAT)
        angles = wavenum.astype(jnp.float32) * (TURN / LAT)
        cosine = jnp.cos(angles)[:, None, None]
        sines = jnp.sin(angles)[:, None, None]
        turned_real = cosine * real_part - sines * imag_part
        turned_imag = sines * real_part + cosine * imag_part
        upper_rows = jnp.concatenate([turned_real, turned_imag], axis=-1)
        lower_rows = jnp.concatenate([turned_imag, -turned_real], axis=-1)
        phased = jnp.stack([upper_rows, lower_rows], axis=2).reshape(site_count * 6, 2 * vectors).astype(jnp.bfloat16)
        results.append(jnp.dot(conj_left.T, phased, preferred_element_type=jnp.float32))
    return jnp.stack(results)


def one_pair(inputs):
    sink_block, source_block, tau = inputs
    vectors = tau.shape[0]
    moms = sink_block.shape[0]
    share_rows = sink_block.shape[1]
    parts = tau.reshape(vectors, 16, 2, vectors)
    lower = jnp.stack([-parts[:, :, 1], parts[:, :, 0]], axis=2).reshape(vectors, 32 * vectors)
    right_side = jnp.concatenate([tau, lower], axis=0)
    left_side = sink_block.reshape(moms * share_rows, 2 * vectors)
    halfway = jnp.dot(left_side.astype(jnp.float32), right_side.astype(jnp.float32)).astype(jnp.bfloat16)
    halfway = halfway.reshape(moms, share_rows * 16, 2 * vectors)
    source_parts = source_block.reshape(moms, vectors, 2, vectors)
    swapped = jnp.stack([-source_parts[:, :, 1], source_parts[:, :, 0]], axis=2).reshape(moms, vectors, 2 * vectors)
    conjugate = jnp.stack([source_block, swapped], axis=1).reshape(moms, 2 * vectors, 2 * vectors)
    loops = jnp.einsum("pmx,pnx->pmn", halfway.astype(jnp.float32), conjugate.astype(jnp.float32))
    return loops.astype(jnp.bfloat16).reshape(moms, share_rows, 16, 2 * vectors)


def reference(eigenvectors, momenta, time_pairs, slot_map, perambulators):
    summed = lax.map(lambda time_slab: elemental(time_slab, momenta, 0), eigenvectors)
    elements = summed.astype(jnp.bfloat16)
    sink_full = elements[slot_map[time_pairs[:, 0]]]
    source_full = elements[slot_map[time_pairs[:, 1]]]
    return lax.map(one_pair, (sink_full, source_full, perambulators))
```

```python
import functools

import jax
import jax.numpy as jnp
from jax import lax
from jax.experimental import pallas as pl
from jax.experimental.pallas import tpu as pltpu
from jax.sharding import PartitionSpec as P

LAT = 32
TURN = 6.283185307179586
SPINS = 16
SHARE = ("space", "spin")
SMEM = pl.BlockSpec(memory_space=pltpu.SMEM)
VMEM = pl.BlockSpec(memory_space=pltpu.VMEM)


def swapped(value, first, second):
    half = value.shape[1] // 2
    lane = lax.broadcasted_iota(jnp.int32, value.shape, 1)
    sign = jnp.where(lane < half, first, second).astype(jnp.float32)
    return pltpu.roll(value.astype(jnp.float32), half, 1) * sign


def elementals_kernel(pos_ref, mom_ref, x_hbm, *rest, groups, chunk):
    outs = rest[:groups]
    x_ref, table_ref, phased_ref, part_ref, sems = rest[groups:]
    slots, colours, sites, width = x_ref.shape
    half = width // 2
    moms = mom_ref.shape[1]
    rows = half // groups
    copies = [pltpu.make_async_copy(x_hbm.at[s], x_ref.at[s], sems.at[s]) for s in range(slots)]
    for copy in copies:
        copy.start()
    pos = pos_ref[0]
    row = lax.broadcasted_iota(jnp.int32, (moms, sites), 0)
    site = lax.broadcasted_iota(jnp.int32, (moms, sites), 1) + pos * sites
    coords = (site % LAT, site // LAT % LAT, site // (LAT * LAT))
    wave = jnp.zeros((moms, sites), jnp.int32)
    for d in range(3):
        value = jnp.zeros((moms, sites), jnp.int32)
        for m in range(moms):
            value = jnp.where(row == m, mom_ref[d, m], value)
        wave = wave + value * coords[d]
    angle = (wave & (LAT - 1)).astype(jnp.float32) * (TURN / LAT)
    table_ref[...] = jnp.concatenate([jnp.cos(angle), jnp.sin(angle)], axis=0).T
    for copy in copies:
        copy.wait()

    def step(i, carry):
        at = pl.ds(pl.multiple_of(i * chunk, chunk), chunk)
        table = table_ref[at, :]
        blocks = [(s, c) for s in range(slots) for c in range(colours)]
        plain = [x_ref[s, c, at, :].astype(jnp.float32) for s, c in blocks]
        turned = [swapped(value, -1.0, 1.0) for value in plain]
        for m in range(moms):
            cosine = jnp.broadcast_to(table[:, m : m + 1], (chunk, width))
            sine = jnp.broadcast_to(table[:, moms + m : moms + m + 1], (chunk, width))
            for n, (s, c) in enumerate(blocks):
                phased_ref[s, c, at, m * width : (m + 1) * width] = (
                    cosine * plain[n] + sine * turned[n]
                ).astype(jnp.bfloat16)
        return carry

    lax.fori_loop(0, sites // chunk, step, 0)
    for s in range(slots):
        products = lax.dot_general(
            x_ref[s].reshape(colours * sites, width),
            phased_ref[s].reshape(colours * sites, moms * width),
            (((0,), (0,)), ((), ())),
            preferred_element_type=jnp.float32,
        )
        for m in range(moms):
            block = products[:, m * width : (m + 1) * width]
            value = block[:half] + swapped(block[half:], 1.0, -1.0)
            for r in range(groups):
                part_ref[r, s, m] = value[r * rows : (r + 1) * rows]
    for j in range(groups):
        outs[j][...] = part_ref[lax.rem(pos + j, groups)].astype(outs[j].dtype)


def elementals(pos, mom_t, x, groups, chunk=16):
    slots, colours, sites, width = x.shape
    moms = mom_t.shape[1]
    rows = width // 2 // groups
    shape = (slots, moms, rows, width)
    return pl.pallas_call(
        functools.partial(elementals_kernel, groups=groups, chunk=chunk),
        out_shape=[jax.ShapeDtypeStruct(shape, jnp.float32)]
        + [jax.ShapeDtypeStruct(shape, jnp.bfloat16)] * (groups - 1),
        in_specs=[SMEM, SMEM, pl.BlockSpec(memory_space=pl.ANY)],
        out_specs=[VMEM] * groups,
        scratch_shapes=[
            pltpu.VMEM((slots, colours, sites, width), jnp.bfloat16),
            pltpu.VMEM((sites, 2 * moms), jnp.float32),
            pltpu.VMEM((slots, colours, sites, moms * width), jnp.bfloat16),
            pltpu.VMEM((groups, slots, moms, rows, width), jnp.float32),
            pltpu.SemaphoreType.DMA((slots,)),
        ],
        compiler_params=pltpu.CompilerParams(vmem_limit_bytes=40 * 1024 * 1024),
        name="elementals",
    )(pos, mom_t, x)


def pick(place_ref, pairs_ref, map_ref, side, k, arrived, store):
    members = len(arrived)
    slots = arrived[0].shape[0]
    slot = map_ref[pairs_ref[side, k]]
    shift = lax.rem(place_ref[1] + members - slot // slots, members)
    for s in range(members):

        @pl.when(shift == s)
        def _():
            store(arrived[s][lax.rem(slot, slots)])


def choose_kernel(place_ref, pairs_ref, map_ref, *rest):
    arrived, out_ref = rest[:-1], rest[-1]
    for k in range(out_ref.shape[0]):

        def store(block):
            out_ref[k] = block

        pick(place_ref, pairs_ref, map_ref, 1, k, arrived, store)


def choose(place, pairs_t, slot_map, arrived):
    shape = (pairs_t.shape[1],) + arrived[0].shape[1:]
    return pl.pallas_call(
        choose_kernel,
        out_shape=jax.ShapeDtypeStruct(shape, arrived[0].dtype),
        in_specs=[SMEM] * 3 + [VMEM] * len(arrived),
        out_specs=VMEM,
        name="choose",
    )(place, pairs_t, slot_map, *arrived)


def halfway_kernel(place_ref, pairs_ref, map_ref, tau_ref, *rest, members):
    arrived = rest[:members]
    out_ref, sink_ref, right_ref, turn_ref = rest[members:]
    k = pl.program_id(0)
    moms, rows, width = sink_ref.shape
    vectors = tau_ref.shape[1]

    def store(block):
        sink_ref[...] = block

    pick(place_ref, pairs_ref, map_ref, 0, k, arrived, store)
    right_ref[:vectors] = tau_ref[0]
    for g in range(SPINS):
        at = slice(g * width, (g + 1) * width)
        right_ref[vectors:, at] = swapped(tau_ref[0, :, at], -1.0, 1.0).astype(jnp.bfloat16)
    product = jnp.dot(
        sink_ref[...].reshape(moms * rows, width),
        right_ref[...],
        preferred_element_type=jnp.float32,
    )
    for g in range(SPINS):
        turn_ref[pl.ds(g, moms * rows, stride=SPINS), :] = product[:, g * width : (g + 1) * width]
    out_ref[0] = turn_ref[...].astype(jnp.bfloat16)


def halfway(place, pairs_t, slot_map, perambulators, arrived):
    pairs, vectors, wide = perambulators.shape
    _, moms, rows, width = arrived[0].shape
    count = moms * rows * SPINS
    return pl.pallas_call(
        functools.partial(halfway_kernel, members=len(arrived)),
        grid=(pairs,),
        out_shape=jax.ShapeDtypeStruct((pairs, count, width), jnp.bfloat16),
        in_specs=[SMEM] * 3
        + [pl.BlockSpec((1, vectors, wide), lambda k: (k, 0, 0))]
        + [VMEM] * len(arrived),
        out_specs=pl.BlockSpec((1, count, width), lambda k: (k, 0, 0)),
        scratch_shapes=[
            pltpu.VMEM((moms, rows, width), jnp.bfloat16),
            pltpu.VMEM((2 * vectors, wide), jnp.bfloat16),
            pltpu.VMEM((count, width), jnp.float32),
        ],
        name="halfway",
    )(place, pairs_t, slot_map, perambulators, *arrived)


def loops_kernel(place_ref, half_ref, *rest, groups):
    sources = rest[:groups]
    out_ref, full_ref = rest[groups:]
    moms, _, rows, width = full_ref.shape
    for j in range(groups):
        full_ref[:, lax.rem(place_ref[0] + groups - j, groups)] = sources[j][0]
    count = rows * SPINS
    for m in range(moms):
        source = full_ref[m].reshape(groups * rows, width)
        right = jnp.concatenate([source, swapped(source, -1.0, 1.0).astype(jnp.bfloat16)], axis=0)
        product = lax.dot_general(
            half_ref[0, m * count : (m + 1) * count],
            right,
            (((1,), (1,)), ((), ())),
            preferred_element_type=jnp.float32,
        )
        out_ref[0, m] = product.astype(jnp.bfloat16).reshape(rows, SPINS, width)


def loops(place, half, sources):
    pairs, count, width = half.shape
    groups = len(sources)
    _, moms, rows, _ = sources[0].shape
    return pl.pallas_call(
        functools.partial(loops_kernel, groups=groups),
        grid=(pairs,),
        out_shape=jax.ShapeDtypeStruct((pairs, moms, rows, SPINS, width), jnp.bfloat16),
        in_specs=[SMEM, pl.BlockSpec((1, count, width), lambda k: (k, 0, 0))]
        + [pl.BlockSpec((1, moms, rows, width), lambda k: (k, 0, 0, 0))] * groups,
        out_specs=pl.BlockSpec((1, moms, rows, SPINS, width), lambda k: (k, 0, 0, 0, 0)),
        scratch_shapes=[pltpu.VMEM((moms, groups, rows, width), jnp.bfloat16)],
        name="loops",
    )(place, half, *sources)


def shifted(value, axes, by):
    size = lax.axis_size(axes)
    return lax.ppermute(value, axes, [(i, (i + by) % size) for i in range(size)])


def per_device(eigenvectors, momenta, time_pairs, slot_map, perambulators):
    groups = lax.axis_size(SHARE)
    members = lax.axis_size("tm")
    place = jnp.stack([lax.axis_index(SHARE), lax.axis_index("tm")]).astype(jnp.int32)
    pairs_t = time_pairs.T
    parts = elementals(place, momenta.T, jnp.transpose(eigenvectors, (0, 2, 1, 3)), groups)
    received = [shifted(parts[j], SHARE, j) for j in range(1, groups)]
    row_share = parts[0]
    for part in received:
        row_share = row_share + part.astype(jnp.float32)
    row_share = row_share.astype(jnp.bfloat16)
    arrived = [row_share] + [shifted(row_share, "tm", j) for j in range(1, members)]
    source_share = choose(place, pairs_t, slot_map, arrived)
    sources = [source_share] + [shifted(source_share, SHARE, j) for j in range(1, groups)]
    half = halfway(place, pairs_t, slot_map, perambulators, arrived)
    return loops(place, half, sources)


def solution(mesh):
    placed = (
        P(("cfg", "tm"), ("space", "spin"), None, None),
        P(),
        P(("cfg", "tm"), None),
        P(),
        P(("cfg", "tm"), None, None),
    )
    return jax.shard_map(
        per_device,
        mesh=mesh,
        in_specs=placed,
        out_specs=P(("cfg", "tm"), None, ("space", "spin"), None, None),
        check_vma=False,
    )
```

```python
import jax
import jax.numpy as jnp
from jax import lax
from jax.experimental import pallas as pl
from jax.experimental.pallas import tpu as pltpu
from jax.sharding import PartitionSpec as P


LAT = 32
TURN = 6.283185307179586
SPINS = 16
SMEM = pl.BlockSpec(memory_space=pltpu.SMEM)
VMEM = pl.BlockSpec(memory_space=pltpu.VMEM)
HBM = pl.BlockSpec(memory_space=pltpu.HBM)
ANY = pl.BlockSpec(memory_space=pl.ANY)


def params(mib):
    return pltpu.CompilerParams(vmem_limit_bytes=mib * 1024 * 1024)


def in_hbm(value):
    return pltpu.with_memory_space_constraint(value, pltpu.HBM)


def swapped(value, first, second):
    half = value.shape[1] // 2
    lane = lax.broadcasted_iota(jnp.int32, value.shape, 1)
    sign = jnp.where(lane < half, first, second).astype(jnp.float32)
    return pltpu.roll(value.astype(jnp.float32), half, 1) * sign


def elementals_kernel(place_hbm, mom_hbm, x_hbm, keep_ref, give_ref, *scratch):
    x_ref, place_ref, mom_ref, table_ref, plain_ref, phased_ref, part_ref, small_sems, sems = scratch
    slots, colours, sites, width = x_ref.shape
    half = width // 2
    moms = mom_ref.shape[1]
    spaces, _, _, rows, _ = keep_ref.shape
    spins = half // (rows * spaces)
    mom_copy = pltpu.make_async_copy(mom_hbm, mom_ref, small_sems.at[0])
    mom_copy.start()
    place_copy = pltpu.make_async_copy(place_hbm, place_ref, small_sems.at[1])
    place_copy.start()
    copies = [pltpu.make_async_copy(x_hbm.at[s], x_ref.at[s], sems.at[s]) for s in range(slots)]
    for copy in copies:
        copy.start()
    row = lax.broadcasted_iota(jnp.int32, (moms, sites), 0)
    site = lax.broadcasted_iota(jnp.int32, (moms, sites), 1)
    place_copy.wait()
    space = place_ref[0]
    spin = place_ref[1]
    site = site + (space * spins + spin) * sites
    coords = (site % LAT, site // LAT % LAT, site // (LAT * LAT))
    mom_copy.wait()
    wave = jnp.zeros((moms, sites), jnp.int32)
    for d in range(3):
        value = jnp.zeros((moms, sites), jnp.int32)
        for m in range(moms):
            value = jnp.where(row == m, mom_ref[d, m], value)
        wave = wave + value * coords[d]
    angle = (wave & (LAT - 1)).astype(jnp.float32) * (TURN / LAT)
    table_ref[0] = jnp.cos(angle)
    table_ref[1] = jnp.sin(angle)
    tiles = sites // width
    pieces = [(c, t) for c in range(colours) for t in range(tiles)]
    for s in range(slots):
        copies[s].wait()
        lefts = []
        for c, t in pieces:
            left = x_ref[s, c, t * width : (t + 1) * width].T
            lefts.append(left)
            plain_ref[s, c, t] = left.astype(jnp.float32)
        left = jnp.concatenate(lefts, axis=1)
        for p in range(moms // 2):
            for i in range(2):
                m = 2 * p + i
                for t in range(tiles):
                    at = slice(t * width, (t + 1) * width)
                    cosine = jnp.broadcast_to(table_ref[0, m : m + 1, at], (half, width))
                    sine = jnp.broadcast_to(table_ref[1, m : m + 1, at], (half, width))
                    for c in range(colours):
                        real = plain_ref[s, c, t, :half]
                        imag = plain_ref[s, c, t, half:]
                        base = i * width
                        phased_ref[s, p, c, t, base : base + half] = (
                            cosine * real - sine * imag
                        ).astype(jnp.bfloat16)
                        phased_ref[s, p, c, t, base + half : base + width] = (
                            sine * real + cosine * imag
                        ).astype(jnp.bfloat16)
            right = jnp.concatenate([phased_ref[s, p, c, t] for c, t in pieces], axis=1)
            products = lax.dot_general(
                left, right, (((1,), (1,)), ((), ())), preferred_element_type=jnp.float32
            )
            for i in range(2):
                block = products[:, i * width : (i + 1) * width]
                value = block[:half] + swapped(block[half:], 1.0, -1.0)
                for r in range(half // rows):
                    part_ref[r // spins, r % spins, s, 2 * p + i] = value[r * rows : (r + 1) * rows]
    for j in range(spaces):
        at = lax.rem(space + j, spaces)
        keep_ref[j] = part_ref[at, spin]
        for i in range(1, spins):
            give_ref[i - 1, j] = part_ref[at, lax.rem(spin + i, spins)]


def elementals(place, mom_t, x, spaces, spins):
    slots, colours, sites, width = x.shape
    moms = mom_t.shape[1]
    shape = (slots, moms, width // 2 // (spaces * spins), width)
    return pl.pallas_call(
        elementals_kernel,
        out_shape=[
            jax.ShapeDtypeStruct((spaces,) + shape, jnp.float32),
            jax.ShapeDtypeStruct((spins - 1, spaces) + shape, jnp.float32),
        ],
        in_specs=[ANY, ANY, ANY],
        out_specs=[VMEM, VMEM],
        scratch_shapes=[
            pltpu.VMEM(x.shape, x.dtype),
            pltpu.SMEM(place.shape, jnp.int32),
            pltpu.SMEM(mom_t.shape, jnp.int32),
            pltpu.VMEM((2, moms, sites), jnp.float32),
            pltpu.VMEM((slots, colours, sites // width, width, width), jnp.float32),
            pltpu.VMEM((slots, moms // 2, colours, sites // width, 2 * width, width), jnp.bfloat16),
            pltpu.VMEM((spaces, spins) + shape, jnp.float32),
            pltpu.SemaphoreType.DMA((2,)),
            pltpu.SemaphoreType.DMA((slots,)),
        ],
        compiler_params=params(24),
        name="elementals",
    )(place, in_hbm(mom_t), in_hbm(x))


def halfway_kernel(sink_ref, tau_ref, out_ref, right_ref, turn_ref):
    pairs, vectors, _ = tau_ref.shape
    _, moms, rows, width = sink_ref.shape
    count = moms * rows

    def step(k, carry):
        right_ref[:vectors] = tau_ref[k]
        for g in range(SPINS):
            at = slice(g * width, (g + 1) * width)
            right_ref[vectors:, at] = swapped(tau_ref[k, :, at], -1.0, 1.0).astype(jnp.bfloat16)
        product = jnp.dot(
            sink_ref[k].reshape(count, width),
            right_ref[...],
            preferred_element_type=jnp.float32,
        )
        for g in range(SPINS):
            turn_ref[pl.ds(g, count, stride=SPINS), :] = product[:, g * width : (g + 1) * width]
        out_ref[k] = turn_ref[...].astype(jnp.bfloat16)
        return carry

    lax.fori_loop(0, pairs, step, 0)


def halfway(sink_rows, perambulators):
    pairs, vectors, wide = perambulators.shape
    _, moms, rows, width = sink_rows.shape
    count = moms * rows * SPINS
    return pl.pallas_call(
        halfway_kernel,
        out_shape=jax.ShapeDtypeStruct((pairs, count, width), jnp.bfloat16),
        in_specs=[VMEM, VMEM],
        out_specs=VMEM,
        scratch_shapes=[
            pltpu.VMEM((2 * vectors, wide), jnp.bfloat16),
            pltpu.VMEM((count, width), jnp.float32),
        ],
        compiler_params=params(12),
        cost_estimate=pl.CostEstimate(
            flops=4 * pairs * moms * rows * vectors * wide, bytes_accessed=4 * 2**20, transcendentals=0
        ),
        name="halfway",
    )(sink_rows, perambulators)


def loops_kernel(place_hbm, half_ref, *rest):
    sources = rest[:-5]
    out_hbm, place_ref, full_ref, stage_ref, sems = rest[-5:]
    pairs, moms, rows, spinors, width = stage_ref.shape
    spaces, spins = full_ref.shape[2:4]
    vectors = width // 2
    count = rows * spinors
    place_copy = pltpu.make_async_copy(place_hbm, place_ref, sems.at[pairs * moms // 2])
    place_copy.start()
    place_copy.wait()
    space = place_ref[0]
    spin = place_ref[1]
    for j in range(spaces):
        for i in range(spins):
            full_ref[
                :, :, lax.rem(space + spaces - j, spaces), lax.rem(spin + spins - i, spins)
            ] = sources[j * spins + i][...]
    copies = []
    zeros = jnp.zeros((width, width), jnp.bfloat16)
    for k in range(pairs):
        for m in range(0, moms, 2):
            rights = []
            for i in range(2):
                source = full_ref[k, m + i].reshape(vectors, width)
                turned = swapped(source, -1.0, 1.0).astype(jnp.bfloat16)
                rights.append(jnp.concatenate([source, turned], axis=0))
            right = jnp.concatenate(
                [
                    jnp.concatenate([rights[0], zeros], axis=1),
                    jnp.concatenate([zeros, rights[1]], axis=1),
                ],
                axis=0,
            )
            left = jnp.concatenate(
                [half_ref[k, (m + i) * count : (m + i + 1) * count] for i in range(2)], axis=1
            )
            product = lax.dot_general(
                left, right, (((1,), (1,)), ((), ())), preferred_element_type=jnp.float32
            ).astype(jnp.bfloat16)
            for i in range(2):
                stage_ref[k, m + i] = product[:, i * width : (i + 1) * width].reshape(
                    rows, spinors, width
                )
            at = pl.ds(m, 2)
            copies.append(
                pltpu.make_async_copy(
                    stage_ref.at[k, at], out_hbm.at[k, at], sems.at[k * moms // 2 + m // 2]
                )
            )
            copies[-1].start()
    for copy in copies:
        copy.wait()


def loops(place, half, sources):
    pairs, _, width = half.shape
    spaces, spins = len(sources), len(sources[0])
    _, moms, rows, _ = sources[0][0].shape
    shape = (pairs, moms, rows, SPINS, width)
    return pl.pallas_call(
        loops_kernel,
        out_shape=jax.ShapeDtypeStruct(shape, jnp.bfloat16),
        in_specs=[ANY, VMEM] + [VMEM] * (spaces * spins),
        out_specs=HBM,
        scratch_shapes=[
            pltpu.SMEM(place.shape, jnp.int32),
            pltpu.VMEM((pairs, moms, spaces, spins, rows, width), jnp.bfloat16),
            pltpu.VMEM(shape, jnp.bfloat16),
            pltpu.SemaphoreType.DMA((pairs * moms // 2 + 1,)),
        ],
        compiler_params=params(16),
        name="loops",
    )(place, half, *[part for group in sources for part in group])


def shifted(value, axis, by):
    size = lax.axis_size(axis)
    return lax.ppermute(value, axis, [(i, (i + by) % size) for i in range(size)])


def around(value, axis):
    parts = [value]
    for j in range(1, lax.axis_size(axis)):
        parts.append(shifted(value, axis, j))
    return parts


def selected(index, candidates):
    flag = index[:, None, None, None]
    result = jnp.broadcast_to(candidates[0], (index.shape[0],) + candidates[0].shape)
    for n in range(1, len(candidates)):
        result = jnp.where(flag == n, candidates[n], result)
    return result


def per_device(eigenvectors, momenta, time_pairs, slot_map, perambulators):
    spaces = lax.axis_size("space")
    spins = lax.axis_size("spin")
    members = lax.axis_size("tm")
    slots = eigenvectors.shape[0]
    place = jnp.stack([lax.axis_index("space"), lax.axis_index("spin")]).astype(jnp.int32)
    times = slot_map.shape[0]
    named = time_pairs[:, :, None] == lax.iota(jnp.int32, times)
    slot = jnp.sum(jnp.where(named, slot_map, 0), axis=-1)
    back = (lax.axis_index("tm") + members - slot // slots) % members
    index = back * slots + slot % slots

    keep, give = elementals(
        place, momenta.T, jnp.transpose(eigenvectors, (0, 2, 1, 3)), spaces, spins
    )
    total = keep
    for i in range(1, spins):
        total = total + shifted(give[i - 1], "spin", i)
    row_share = total[0]
    for j in range(1, spaces):
        row_share = row_share + shifted(total[j].astype(jnp.bfloat16), "space", j).astype(
            jnp.float32
        )
    row_share = row_share.astype(jnp.bfloat16)
    arrived = around(row_share, "tm")
    candidates = [part[s] for part in arrived for s in range(slots)]
    source_share = selected(index[:, 1], candidates)
    sink_rows = selected(index[:, 0], candidates)
    far = around(source_share, "space")
    sources = [around(part, "spin") for part in far]
    half = halfway(sink_rows, perambulators)
    return loops(place, half, sources)


def solution(mesh):
    placed = (
        P(("cfg", "tm"), ("space", "spin"), None, None),
        P(),
        P(("cfg", "tm"), None),
        P(),
        P(("cfg", "tm"), None, None),
    )

    return jax.shard_map(
        per_device,
        mesh=mesh,
        in_specs=placed,
        out_specs=P(("cfg", "tm"), None, ("space", "spin"), None, None),
        check_vma=False,
    )
```

```python
import jax
import jax.numpy as jnp
from jax import lax
from jax.experimental import pallas as pl
from jax.experimental.pallas import tpu as pltpu
from jax.sharding import PartitionSpec as P


LAT = 32
TURN = 6.283185307179586
SPINS = 16
SMEM = pl.BlockSpec(memory_space=pltpu.SMEM)
VMEM = pl.BlockSpec(memory_space=pltpu.VMEM)
HBM = pl.BlockSpec(memory_space=pltpu.HBM)
ANY = pl.BlockSpec(memory_space=pl.ANY)


def params(mib):
    return pltpu.CompilerParams(vmem_limit_bytes=mib * 1024 * 1024)


def in_hbm(value):
    return pltpu.with_memory_space_constraint(value, pltpu.HBM)


def swapped(value, first, second):
    half = value.shape[1] // 2
    lane = lax.broadcasted_iota(jnp.int32, value.shape, 1)
    sign = jnp.where(lane < half, first, second).astype(jnp.float32)
    return pltpu.roll(value.astype(jnp.float32), half, 1) * sign


def turn_and_sum(lefts, table_ref, first, phased_ref, sum_ref):
    slots, colours, _, tiles, _, width = phased_ref.shape
    half = width // 2
    spaces, _, count, rows, _ = sum_ref.shape
    for s in range(slots):
        totals = [None] * (count // 2)
        for c in range(colours):
            left = [lefts(s, c, t) for t in range(tiles)]
            for t in range(tiles):
                at = slice(t * width, (t + 1) * width)
                real = left[t][:half].astype(jnp.float32)
                imag = left[t][half:].astype(jnp.float32)
                for m in range(count):
                    row = slice(first + m, first + m + 1)
                    cosine = jnp.broadcast_to(table_ref[0, row, at], (half, width))
                    sine = jnp.broadcast_to(table_ref[1, row, at], (half, width))
                    top = m % 2 * width
                    phased_ref[s, c, m // 2, t, top : top + half] = (
                        cosine * real - sine * imag
                    ).astype(jnp.bfloat16)
                    phased_ref[s, c, m // 2, t, top + half : top + width] = (
                        sine * real + cosine * imag
                    ).astype(jnp.bfloat16)
            left = jnp.concatenate(left, axis=1)
            for p in range(count // 2):
                right = jnp.concatenate([phased_ref[s, c, p, t] for t in range(tiles)], axis=1)
                product = lax.dot_general(
                    left, right, (((1,), (1,)), ((), ())), preferred_element_type=jnp.float32
                )
                totals[p] = product if totals[p] is None else totals[p] + product
        for m in range(count):
            block = totals[m // 2][:, m % 2 * width : (m % 2 + 1) * width]
            value = block[:half] + swapped(block[half:], 1.0, -1.0)
            for r in range(spaces):
                sum_ref[r, s, m] = value[r * rows : (r + 1) * rows]


def given_kernel(place_hbm, mom_hbm, x_hbm, out_ref, table_ref, turned_ref, *scratch):
    x_ref, place_ref, mom_ref, phased_ref, sum_ref, sems = scratch
    _, _, sites, width = x_ref.shape
    spaces, _, count, _, _ = out_ref.shape
    moms = mom_ref.shape[1]
    spins = moms // count
    x_copy = pltpu.make_async_copy(x_hbm, x_ref, sems.at[0])
    mom_copy = pltpu.make_async_copy(mom_hbm, mom_ref, sems.at[1])
    place_copy = pltpu.make_async_copy(place_hbm, place_ref, sems.at[2])
    mom_copy.start()
    place_copy.start()
    x_copy.start()
    row = lax.broadcasted_iota(jnp.int32, (moms, sites), 0)
    site = lax.broadcasted_iota(jnp.int32, (moms, sites), 1)
    place_copy.wait()
    space = place_ref[0]
    spin = place_ref[1]
    site = site + (space * spins + spin) * sites
    coords = (site % LAT, site // LAT % LAT, site // (LAT * LAT))
    mom_copy.wait()
    wave = jnp.zeros((moms, sites), jnp.int32)
    for d in range(3):
        value = jnp.zeros((moms, sites), jnp.int32)
        for m in range(moms):
            value = jnp.where(
                row == m, mom_ref[d, lax.rem(spin + m // count, spins) * count + m % count], value
            )
        wave = wave + value * coords[d]
    angle = (wave & (LAT - 1)).astype(jnp.float32) * (TURN / LAT)
    table_ref[0] = jnp.cos(angle)
    table_ref[1] = jnp.sin(angle)
    x_copy.wait()

    def lefts(s, c, t):
        value = x_ref[s, c, t * width : (t + 1) * width].T
        turned_ref[s, c, t] = value
        return value

    turn_and_sum(lefts, table_ref, count, phased_ref, sum_ref)
    for j in range(spaces):
        out_ref[j] = sum_ref[lax.rem(space + j, spaces)]


def given(place, mom_t, x, spaces, spins):
    slots, colours, sites, width = x.shape
    moms = mom_t.shape[1]
    count = moms // spins
    shape = (spaces, slots, count, width // 2 // spaces, width)
    tiles = sites // width
    return pl.pallas_call(
        given_kernel,
        out_shape=[
            jax.ShapeDtypeStruct(shape, jnp.float32),
            jax.ShapeDtypeStruct((2, moms, sites), jnp.float32),
            jax.ShapeDtypeStruct((slots, colours, tiles, width, width), x.dtype),
        ],
        in_specs=[ANY, ANY, ANY],
        out_specs=[VMEM] * 3,
        scratch_shapes=[
            pltpu.VMEM(x.shape, x.dtype),
            pltpu.SMEM(place.shape, jnp.int32),
            pltpu.SMEM(mom_t.shape, jnp.int32),
            pltpu.VMEM((slots, colours, count // 2, tiles, 2 * width, width), jnp.bfloat16),
            pltpu.VMEM(shape, jnp.float32),
            pltpu.SemaphoreType.DMA((3,)),
        ],
        compiler_params=params(20),
        name="given",
    )(place, in_hbm(mom_t), in_hbm(x))


def kept_kernel(place_hbm, table_ref, turned_ref, out_ref, place_ref, phased_ref, sum_ref, sem):
    spaces = out_ref.shape[0]
    place_copy = pltpu.make_async_copy(place_hbm, place_ref, sem)
    place_copy.start()
    turn_and_sum(lambda s, c, t: turned_ref[s, c, t], table_ref, 0, phased_ref, sum_ref)
    place_copy.wait()
    for j in range(spaces):
        out_ref[j] = sum_ref[lax.rem(place_ref[0] + j, spaces)]


def kept(place, table, turned, spaces, spins):
    slots, colours, tiles, width, _ = turned.shape
    count = table.shape[1] // spins
    shape = (spaces, slots, count, width // 2 // spaces, width)
    return pl.pallas_call(
        kept_kernel,
        out_shape=jax.ShapeDtypeStruct(shape, jnp.float32),
        in_specs=[ANY, VMEM, VMEM],
        out_specs=VMEM,
        scratch_shapes=[
            pltpu.SMEM(place.shape, jnp.int32),
            pltpu.VMEM((slots, colours, count // 2, tiles, 2 * width, width), jnp.bfloat16),
            pltpu.VMEM(shape, jnp.float32),
            pltpu.SemaphoreType.DMA,
        ],
        compiler_params=params(20),
        name="kept",
    )(place, table, turned)


def doubled_kernel(tau_ref, out_ref):
    pairs, vectors, wide = tau_ref.shape
    width = 2 * vectors
    for k in range(pairs):
        out_ref[k, :vectors] = tau_ref[k]
        for g in range(wide // width):
            at = slice(g * width, (g + 1) * width)
            out_ref[k, vectors:, at] = swapped(tau_ref[k, :, at], -1.0, 1.0).astype(jnp.bfloat16)


def doubled(perambulators):
    pairs, vectors, wide = perambulators.shape
    return pl.pallas_call(
        doubled_kernel,
        out_shape=jax.ShapeDtypeStruct((pairs, 2 * vectors, wide), perambulators.dtype),
        in_specs=[VMEM],
        out_specs=VMEM,
        compiler_params=params(8),
        name="doubled",
    )(perambulators)


def halfway_kernel(right_ref, *rest):
    sinks, out_ref, turn_ref = rest[:-2], rest[-2], rest[-1]
    pairs, count, rows, width = sinks[0].shape
    lines = len(sinks) * count * rows

    def step(k, carry):
        left = jnp.concatenate([sink[k].reshape(count * rows, width) for sink in sinks], axis=0)
        product = jnp.dot(left, right_ref[k], preferred_element_type=jnp.float32)
        for g in range(SPINS):
            turn_ref[pl.ds(g, lines, stride=SPINS), :] = product[:, g * width : (g + 1) * width]
        out_ref[k] = turn_ref[...].astype(jnp.bfloat16)
        return carry

    lax.fori_loop(0, pairs, step, 0)


def halfway(right, sinks):
    pairs, count, rows, width = sinks[0].shape
    lines = len(sinks) * count * rows * SPINS
    return pl.pallas_call(
        halfway_kernel,
        out_shape=jax.ShapeDtypeStruct((pairs, lines, width), jnp.bfloat16),
        in_specs=[VMEM] * (1 + len(sinks)),
        out_specs=VMEM,
        scratch_shapes=[pltpu.VMEM((lines, width), jnp.float32)],
        compiler_params=params(8),
        name="halfway",
    )(right, *sinks)


def loops_kernel(place_hbm, half_ref, *rest):
    sources = rest[:-5]
    out_hbm, place_ref, full_ref, stage_ref, sems = rest[-5:]
    pairs, moms, rows, spinors, width = stage_ref.shape
    _, _, spaces, _, _ = full_ref.shape
    spins = len(sources) // spaces
    part = moms // spins
    vectors = width // 2
    count = rows * spinors
    place_copy = pltpu.make_async_copy(place_hbm, place_ref, sems.at[pairs * moms // 2])
    place_copy.start()
    place_copy.wait()
    space = place_ref[0]
    spin = place_ref[1]
    for i in range(spins):
        for j in range(spaces):
            full_ref[:, i * part : (i + 1) * part, lax.rem(space + spaces - j, spaces)] = sources[
                i * spaces + j
            ][...]
    copies = []
    zeros = jnp.zeros((width, width), jnp.bfloat16)
    for k in range(pairs):
        for m in range(0, moms, 2):
            rights = []
            for i in range(2):
                source = full_ref[k, m + i].reshape(vectors, width)
                turned = swapped(source, -1.0, 1.0).astype(jnp.bfloat16)
                rights.append(jnp.concatenate([source, turned], axis=0))
            right = jnp.concatenate(
                [
                    jnp.concatenate([rights[0], zeros], axis=1),
                    jnp.concatenate([zeros, rights[1]], axis=1),
                ],
                axis=0,
            )
            left = jnp.concatenate(
                [half_ref[k, (m + i) * count : (m + i + 1) * count] for i in range(2)], axis=1
            )
            product = lax.dot_general(
                left, right, (((1,), (1,)), ((), ())), preferred_element_type=jnp.float32
            ).astype(jnp.bfloat16)
            for i in range(2):
                stage_ref[k, m + i] = product[:, i * width : (i + 1) * width].reshape(
                    rows, spinors, width
                )
            first = lax.rem(spin + spins - m // part, spins) * part + m % part
            copies.append(
                pltpu.make_async_copy(
                    stage_ref.at[k, pl.ds(m, 2)],
                    out_hbm.at[k, pl.ds(first, 2)],
                    sems.at[k * moms // 2 + m // 2],
                )
            )
            copies[-1].start()
    for copy in copies:
        copy.wait()


def loops(place, half, sources):
    pairs, lines, width = half.shape
    spins, spaces = len(sources), len(sources[0])
    _, part, block, _ = sources[0][0].shape
    moms = spins * part
    shape = (pairs, moms, lines // (moms * SPINS), SPINS, width)
    return pl.pallas_call(
        loops_kernel,
        out_shape=jax.ShapeDtypeStruct(shape, jnp.bfloat16),
        in_specs=[ANY, VMEM] + [VMEM] * (spaces * spins),
        out_specs=HBM,
        scratch_shapes=[
            pltpu.SMEM(place.shape, jnp.int32),
            pltpu.VMEM((pairs, moms, spaces, block, width), jnp.bfloat16),
            pltpu.VMEM(shape, jnp.bfloat16),
            pltpu.SemaphoreType.DMA((pairs * moms // 2 + 1,)),
        ],
        compiler_params=params(16),
        name="loops",
    )(place, half, *[block for group in sources for block in group])


def shifted(value, axis, by):
    size = lax.axis_size(axis)
    return lax.ppermute(value, axis, [(i, (i + by) % size) for i in range(size)])


def around(value, axis):
    parts = [value]
    for j in range(1, lax.axis_size(axis)):
        parts.append(shifted(value, axis, j))
    return parts


def across(value, axis):
    size = lax.axis_size(axis)
    parts = [value]
    for j in range(1, size):
        parts.append(lax.ppermute(value, axis, [(i, i ^ j) for i in range(size)]))
    return parts


def selected(index, candidates):
    flag = index[:, None, None, None]
    result = jnp.broadcast_to(candidates[0], (index.shape[0],) + candidates[0].shape)
    for n in range(1, len(candidates)):
        result = jnp.where(flag == n, candidates[n], result)
    return result


def per_device(eigenvectors, momenta, time_pairs, slot_map, perambulators):
    spaces = lax.axis_size("space")
    spins = lax.axis_size("spin")
    slots = eigenvectors.shape[0]
    place = jnp.stack([lax.axis_index("space"), lax.axis_index("spin")]).astype(jnp.int32)
    times = slot_map.shape[0]
    named = time_pairs[:, :, None] == lax.iota(jnp.int32, times)
    slot = jnp.sum(jnp.where(named, slot_map, 0), axis=-1)
    index = (lax.axis_index("tm") ^ slot // slots) * slots + slot % slots

    spin = lax.axis_index("spin")
    x = jnp.transpose(eigenvectors, (0, 2, 1, 3))
    send, table, turned = given(place, momenta.T, x, spaces, spins)
    received = shifted(send, "spin", 1)
    total = kept(place, table, turned, spaces, spins)
    total = total + received
    row_share = total[0]
    for j in range(1, spaces):
        value = shifted(total[j].astype(jnp.bfloat16), "space", j)
        row_share = row_share + value.astype(jnp.float32)
    row_share = row_share.astype(jnp.bfloat16)
    arrived = across(row_share, "tm")
    candidates = [value[s] for value in arrived for s in range(slots)]
    source_share = selected(index[:, 1], candidates)
    sink_share = selected(index[:, 0], candidates)
    rows = sink_share.shape[2] // spins
    sinks = []
    for i in range(spins):
        block = lax.dynamic_slice_in_dim(sink_share, (spin + i) % spins * rows, rows, axis=2)
        if i:
            block = shifted(block, "spin", i)
        sinks.append(block)
    right = doubled(perambulators)
    half = halfway(right, sinks)
    far = around(source_share, "space")
    near = [around(value, "spin") for value in far]
    sources = [[group[i] for group in near] for i in range(spins)]
    return loops(place, half, sources)


def solution(mesh):
    placed = (
        P(("cfg", "tm"), ("space", "spin"), None, None),
        P(),
        P(("cfg", "tm"), None),
        P(),
        P(("cfg", "tm"), None, None),
    )

    members = mesh.shape["tm"]
    order = [j for j in range(1, members) if j & (j + 1) == 0][::-1]
    order += [j for j in range(1, members) if j not in order]
    return jax.shard_map(
        per_device,
        mesh=mesh,
        in_specs=placed,
        out_specs=P(("cfg", "tm"), None, ("space", "spin"), None, None),
        check_vma=False,
    )
```

```python
import functools

import jax
import jax.numpy as jnp
from jax import lax
from jax.experimental import pallas as pl
from jax.experimental.pallas import tpu as pltpu
from jax.sharding import PartitionSpec as P


LAT = 32
TURN = 6.283185307179586
SPINS = 16
SMEM = pl.BlockSpec(memory_space=pltpu.SMEM)
VMEM = pl.BlockSpec(memory_space=pltpu.VMEM)
HBM = pl.BlockSpec(memory_space=pltpu.HBM)
ANY = pl.BlockSpec(memory_space=pl.ANY)


def params(mib):
    return pltpu.CompilerParams(vmem_limit_bytes=mib * 1024 * 1024)


def in_hbm(value):
    return pltpu.with_memory_space_constraint(value, pltpu.HBM)


def swapped(value, first, second):
    half = value.shape[1] // 2
    lane = lax.broadcasted_iota(jnp.int32, value.shape, 1)
    sign = jnp.where(lane < half, first, second).astype(jnp.float32)
    return pltpu.roll(value.astype(jnp.float32), half, 1) * sign


def turn_and_sum(lefts, table_ref, first, phased_ref, sum_ref):
    slots, colours, _, tiles, _, width = phased_ref.shape
    half = width // 2
    spaces, _, count, rows, _ = sum_ref.shape
    for s in range(slots):
        totals = [None] * (count // 2)
        for c in range(colours):
            left = [lefts(s, c, t) for t in range(tiles)]
            for t in range(tiles):
                at = slice(t * width, (t + 1) * width)
                real = left[t][:half].astype(jnp.float32)
                imag = left[t][half:].astype(jnp.float32)
                for m in range(count):
                    row = slice(first + m, first + m + 1)
                    cosine = jnp.broadcast_to(table_ref[0, row, at], (half, width))
                    sine = jnp.broadcast_to(table_ref[1, row, at], (half, width))
                    top = m % 2 * width
                    phased_ref[s, c, m // 2, t, top : top + half] = (
                        cosine * real - sine * imag
                    ).astype(jnp.bfloat16)
                    phased_ref[s, c, m // 2, t, top + half : top + width] = (
                        sine * real + cosine * imag
                    ).astype(jnp.bfloat16)
            left = jnp.concatenate(left, axis=1)
            for p in range(count // 2):
                right = jnp.concatenate([phased_ref[s, c, p, t] for t in range(tiles)], axis=1)
                product = lax.dot_general(
                    left, right, (((1,), (1,)), ((), ())), preferred_element_type=jnp.float32
                )
                totals[p] = product if totals[p] is None else totals[p] + product
        for m in range(count):
            block = totals[m // 2][:, m % 2 * width : (m % 2 + 1) * width]
            value = block[:half] + swapped(block[half:], 1.0, -1.0)
            for r in range(spaces):
                sum_ref[r, s, m] = value[r * rows : (r + 1) * rows]


def given_kernel(place_hbm, mom_hbm, x_hbm, out_ref, table_ref, turned_ref, *scratch):
    x_ref, place_ref, mom_ref, phased_ref, sum_ref, sems = scratch
    _, _, sites, width = x_ref.shape
    spaces, _, count, _, _ = out_ref.shape
    moms = mom_ref.shape[1]
    spins = moms // count
    x_copy = pltpu.make_async_copy(x_hbm, x_ref, sems.at[0])
    mom_copy = pltpu.make_async_copy(mom_hbm, mom_ref, sems.at[1])
    place_copy = pltpu.make_async_copy(place_hbm, place_ref, sems.at[2])
    mom_copy.start()
    place_copy.start()
    x_copy.start()
    row = lax.broadcasted_iota(jnp.int32, (moms, sites), 0)
    site = lax.broadcasted_iota(jnp.int32, (moms, sites), 1)
    place_copy.wait()
    space = place_ref[0]
    spin = place_ref[1]
    site = site + (space * spins + spin) * sites
    coords = (site % LAT, site // LAT % LAT, site // (LAT * LAT))
    mom_copy.wait()
    wave = jnp.zeros((moms, sites), jnp.int32)
    for d in range(3):
        value = jnp.zeros((moms, sites), jnp.int32)
        for m in range(moms):
            value = jnp.where(
                row == m, mom_ref[d, lax.rem(spin + m // count, spins) * count + m % count], value
            )
        wave = wave + value * coords[d]
    angle = (wave & (LAT - 1)).astype(jnp.float32) * (TURN / LAT)
    table_ref[0] = jnp.cos(angle)
    table_ref[1] = jnp.sin(angle)
    x_copy.wait()

    def lefts(s, c, t):
        value = x_ref[s, c, t * width : (t + 1) * width].T
        turned_ref[s, c, t] = value
        return value

    turn_and_sum(lefts, table_ref, count, phased_ref, sum_ref)
    for j in range(spaces):
        out_ref[j] = sum_ref[lax.rem(space + j, spaces)]


def given(place, mom_t, x, spaces, spins):
    slots, colours, sites, width = x.shape
    moms = mom_t.shape[1]
    count = moms // spins
    shape = (spaces, slots, count, width // 2 // spaces, width)
    tiles = sites // width
    return pl.pallas_call(
        given_kernel,
        out_shape=[
            jax.ShapeDtypeStruct(shape, jnp.float32),
            jax.ShapeDtypeStruct((2, moms, sites), jnp.float32),
            jax.ShapeDtypeStruct((slots, colours, tiles, width, width), x.dtype),
        ],
        in_specs=[ANY, ANY, ANY],
        out_specs=[VMEM] * 3,
        scratch_shapes=[
            pltpu.VMEM(x.shape, x.dtype),
            pltpu.SMEM(place.shape, jnp.int32),
            pltpu.SMEM(mom_t.shape, jnp.int32),
            pltpu.VMEM((slots, colours, count // 2, tiles, 2 * width, width), jnp.bfloat16),
            pltpu.VMEM(shape, jnp.float32),
            pltpu.SemaphoreType.DMA((3,)),
        ],
        compiler_params=params(20),
        name="given",
    )(place, in_hbm(mom_t), in_hbm(x))


def kept_kernel(place_hbm, table_ref, turned_ref, out_ref, place_ref, phased_ref, sum_ref, sem):
    spaces = out_ref.shape[0]
    place_copy = pltpu.make_async_copy(place_hbm, place_ref, sem)
    place_copy.start()
    turn_and_sum(lambda s, c, t: turned_ref[s, c, t], table_ref, 0, phased_ref, sum_ref)
    place_copy.wait()
    for j in range(spaces):
        out_ref[j] = sum_ref[lax.rem(place_ref[0] + j, spaces)]


def kept(place, table, turned, spaces, spins):
    slots, colours, tiles, width, _ = turned.shape
    count = table.shape[1] // spins
    shape = (spaces, slots, count, width // 2 // spaces, width)
    return pl.pallas_call(
        kept_kernel,
        out_shape=jax.ShapeDtypeStruct(shape, jnp.float32),
        in_specs=[ANY, VMEM, VMEM],
        out_specs=VMEM,
        scratch_shapes=[
            pltpu.SMEM(place.shape, jnp.int32),
            pltpu.VMEM((slots, colours, count // 2, tiles, 2 * width, width), jnp.bfloat16),
            pltpu.VMEM(shape, jnp.float32),
            pltpu.SemaphoreType.DMA,
        ],
        compiler_params=params(20),
        name="kept",
    )(place, table, turned)


def doubled_kernel(tau_ref, out_ref):
    pairs, vectors, wide = tau_ref.shape
    width = 2 * vectors
    for k in range(pairs):
        out_ref[k, :vectors] = tau_ref[k]
        for g in range(wide // width):
            at = slice(g * width, (g + 1) * width)
            out_ref[k, vectors:, at] = swapped(tau_ref[k, :, at], -1.0, 1.0).astype(jnp.bfloat16)


def doubled(perambulators):
    pairs, vectors, wide = perambulators.shape
    return pl.pallas_call(
        doubled_kernel,
        out_shape=jax.ShapeDtypeStruct((pairs, 2 * vectors, wide), perambulators.dtype),
        in_specs=[VMEM],
        out_specs=VMEM,
        compiler_params=params(8),
        name="doubled",
    )(perambulators)


def halfway_kernel(right_ref, *rest):
    sinks, out_ref, turn_ref = rest[:-2], rest[-2], rest[-1]
    pairs, count, rows, width = sinks[0].shape
    lines = len(sinks) * count * rows

    def step(k, carry):
        left = jnp.concatenate([sink[k].reshape(count * rows, width) for sink in sinks], axis=0)
        product = jnp.dot(left, right_ref[k], preferred_element_type=jnp.float32)
        for g in range(SPINS):
            turn_ref[pl.ds(g, lines, stride=SPINS), :] = product[:, g * width : (g + 1) * width]
        out_ref[k] = turn_ref[...].astype(jnp.bfloat16)
        return carry

    lax.fori_loop(0, pairs, step, 0)


def halfway(right, sinks):
    pairs, count, rows, width = sinks[0].shape
    lines = len(sinks) * count * rows * SPINS
    return pl.pallas_call(
        halfway_kernel,
        out_shape=jax.ShapeDtypeStruct((pairs, lines, width), jnp.bfloat16),
        in_specs=[VMEM] * (1 + len(sinks)),
        out_specs=VMEM,
        scratch_shapes=[pltpu.VMEM((lines, width), jnp.float32)],
        compiler_params=params(8),
        name="halfway",
    )(right, *sinks)


def loops_kernel(place_hbm, space_ref, half_ref, *rest, spaces):
    sources = rest[:-4]
    out_hbm, place_ref, stage_ref, sems = rest[-4:]
    pairs, moms, rows, spinors, width = stage_ref.shape
    spins = len(sources) // spaces
    part = moms // spins
    block = sources[0].shape[2]
    count = rows * spinors
    place_copy = pltpu.make_async_copy(place_hbm, place_ref, sems.at[1])
    place_copy.start()
    here = [
        jnp.broadcast_to(space_ref[...], (block, width)) == space for space in range(spaces)
    ]
    zeros = jnp.zeros((width, width), jnp.bfloat16)
    for k in range(pairs):
        for m in range(0, moms, 2):
            rights = []
            for i in range(2):
                given_blocks = [
                    sources[(m + i) // part * spaces + j][k, (m + i) % part].astype(jnp.float32)
                    for j in range(spaces)
                ]
                ordered = []
                for r in range(spaces):
                    value = given_blocks[0]
                    for j in range(1, spaces):
                        value = jnp.where(here[(r + j) % spaces], given_blocks[j], value)
                    ordered.append(value)
                source = jnp.concatenate(ordered, axis=0)
                turned = swapped(source, -1.0, 1.0)
                rights.append(jnp.concatenate([source, turned], axis=0).astype(jnp.bfloat16))
            right = jnp.concatenate(
                [
                    jnp.concatenate([rights[0], zeros], axis=1),
                    jnp.concatenate([zeros, rights[1]], axis=1),
                ],
                axis=0,
            )
            left = jnp.concatenate(
                [half_ref[k, (m + i) * count : (m + i + 1) * count] for i in range(2)], axis=1
            )
            product = lax.dot_general(
                left, right, (((1,), (1,)), ((), ())), preferred_element_type=jnp.float32
            ).astype(jnp.bfloat16)
            for i in range(2):
                stage_ref[k, m + i] = product[:, i * width : (i + 1) * width].reshape(
                    rows, spinors, width
                )
            if k == 0 and m == 0:
                place_copy.wait()
                spin = place_ref[1]
            if (m + 2) % part == 0:
                owner = lax.rem(spin + spins - m // part, spins)
                pltpu.make_async_copy(
                    stage_ref.at[k, pl.ds(m + 2 - part, part)],
                    out_hbm.at[k, pl.ds(owner * part, part)],
                    sems.at[0],
                ).start()
    pltpu.make_async_copy(stage_ref, out_hbm, sems.at[0]).wait()


def loops(place, space_row, half, sources):
    pairs, lines, width = half.shape
    spins, spaces = len(sources), len(sources[0])
    _, part, _, _ = sources[0][0].shape
    moms = spins * part
    shape = (pairs, moms, lines // (moms * SPINS), SPINS, width)
    return pl.pallas_call(
        functools.partial(loops_kernel, spaces=spaces),
        out_shape=jax.ShapeDtypeStruct(shape, jnp.bfloat16),
        in_specs=[ANY, VMEM, VMEM] + [VMEM] * (spaces * spins),
        out_specs=HBM,
        scratch_shapes=[
            pltpu.SMEM(place.shape, jnp.int32),
            pltpu.VMEM(shape, jnp.bfloat16),
            pltpu.SemaphoreType.DMA((2,)),
        ],
        compiler_params=params(16),
        name="loops",
    )(place, space_row, half, *[block for group in sources for block in group])


def shifted(value, axis, by):
    size = lax.axis_size(axis)
    return lax.ppermute(value, axis, [(i, (i + by) % size) for i in range(size)])


def around(value, axis):
    parts = [value]
    for j in range(1, lax.axis_size(axis)):
        parts.append(shifted(value, axis, j))
    return parts


def targets(size):
    ring = [0, *range(1, size, 2), *reversed(range(2, size, 2))]
    place = {member: n for n, member in enumerate(ring)}
    return [[ring[(place[i] + j) % size] for i in range(size)] for j in range(1, size)]


def exchanged(value, axis):
    parts = [value]
    for to in targets(lax.axis_size(axis)):
        parts.append(lax.ppermute(value, axis, list(enumerate(to))))
    return parts


def arrivals(size):
    table = [[0] * size for _ in range(size)]
    for n, to in enumerate(targets(size)):
        for sender, receiver in enumerate(to):
            table[receiver][sender] = n + 1
    return table


def selected(index, candidates):
    flag = index[:, None, None, None]
    result = jnp.broadcast_to(candidates[0], (index.shape[0],) + candidates[0].shape)
    for n in range(1, len(candidates)):
        result = jnp.where(flag == n, candidates[n], result)
    return result


def per_device(eigenvectors, momenta, time_pairs, slot_map, perambulators):
    spaces = lax.axis_size("space")
    spins = lax.axis_size("spin")
    slots = eigenvectors.shape[0]
    place = jnp.stack([lax.axis_index("space"), lax.axis_index("spin")]).astype(jnp.int32)
    times = slot_map.shape[0]
    named = time_pairs[:, :, None] == lax.iota(jnp.int32, times)
    slot = jnp.sum(jnp.where(named, slot_map, 0), axis=-1)
    members = lax.axis_size("tm")
    table = jnp.array(arrivals(members), jnp.int32)
    row = jnp.sum(
        jnp.where((lax.iota(jnp.int32, members) == lax.axis_index("tm"))[:, None], table, 0), 0
    )
    held = (slot // slots)[..., None] == lax.iota(jnp.int32, members)
    index = jnp.sum(jnp.where(held, row, 0), axis=-1) * slots + slot % slots

    spin = lax.axis_index("spin")
    x = jnp.transpose(eigenvectors, (0, 2, 1, 3))
    send, table, turned = given(place, momenta.T, x, spaces, spins)
    received = shifted(send, "spin", 1)
    total = kept(place, table, turned, spaces, spins)
    total = total + received
    row_share = total[0]
    for j in range(1, spaces):
        value = shifted(total[j].astype(jnp.bfloat16), "space", j)
        row_share = row_share + value.astype(jnp.float32)
    row_share = row_share.astype(jnp.bfloat16)
    arrived = exchanged(row_share, "tm")
    candidates = [value[s] for value in arrived for s in range(slots)]
    source_share = selected(index[:, 1], candidates)
    sink_share = selected(index[:, 0], candidates)
    rows = sink_share.shape[2] // spins
    sinks = []
    for i in range(spins):
        block = lax.dynamic_slice_in_dim(sink_share, (spin + i) % spins * rows, rows, axis=2)
        if i:
            block = shifted(block, "spin", i)
        sinks.append(block)
    right = doubled(perambulators)
    half = halfway(right, sinks)
    far = around(source_share, "space")
    near = [around(value, "spin") for value in far]
    sources = [[group[i] for group in near] for i in range(spins)]
    space_row = jnp.full((1, perambulators.shape[1] * 2), lax.axis_index("space"), jnp.int32)
    return loops(place, space_row, half, sources)


def solution(mesh):
    placed = (
        P(("cfg", "tm"), ("space", "spin"), None, None),
        P(),
        P(("cfg", "tm"), None),
        P(),
        P(("cfg", "tm"), None, None),
    )

    return jax.shard_map(
        per_device,
        mesh=mesh,
        in_specs=placed,
        out_specs=P(("cfg", "tm"), None, ("space", "spin"), None, None),
        check_vma=False,
    )
```

```python
import functools

import jax
import jax.numpy as jnp
from jax import lax
from jax.experimental import pallas as pl
from jax.experimental.pallas import tpu as pltpu
from jax.sharding import PartitionSpec as P


LAT = 32
TURN = 6.283185307179586
SPINS = 16
SMEM = pl.BlockSpec(memory_space=pltpu.SMEM)
VMEM = pl.BlockSpec(memory_space=pltpu.VMEM)
HBM = pl.BlockSpec(memory_space=pltpu.HBM)
ANY = pl.BlockSpec(memory_space=pl.ANY)


def params(mib):
    return pltpu.CompilerParams(vmem_limit_bytes=mib * 1024 * 1024)


def in_hbm(value):
    return pltpu.with_memory_space_constraint(value, pltpu.HBM)


def swapped(value, first, second):
    half = value.shape[1] // 2
    lane = lax.broadcasted_iota(jnp.int32, value.shape, 1)
    sign = jnp.where(lane < half, first, second).astype(jnp.float32)
    return pltpu.roll(value.astype(jnp.float32), half, 1) * sign


def turn_and_sum(lefts, table_ref, first, phased_ref, sum_ref):
    slots, colours, _, tiles, _, width = phased_ref.shape
    half = width // 2
    spaces, _, count, rows, _ = sum_ref.shape
    for s in range(slots):
        totals = [None] * (count // 2)
        for c in range(colours):
            left = [lefts(s, c, t) for t in range(tiles)]
            for t in range(tiles):
                at = slice(t * width, (t + 1) * width)
                real = left[t][:half].astype(jnp.float32)
                imag = left[t][half:].astype(jnp.float32)
                for m in range(count):
                    row = slice(first + m, first + m + 1)
                    cosine = jnp.broadcast_to(table_ref[0, row, at], (half, width))
                    sine = jnp.broadcast_to(table_ref[1, row, at], (half, width))
                    top = m % 2 * width
                    phased_ref[s, c, m // 2, t, top : top + half] = (
                        cosine * real - sine * imag
                    ).astype(jnp.bfloat16)
                    phased_ref[s, c, m // 2, t, top + half : top + width] = (
                        sine * real + cosine * imag
                    ).astype(jnp.bfloat16)
            left = jnp.concatenate(left, axis=1)
            for p in range(count // 2):
                right = jnp.concatenate([phased_ref[s, c, p, t] for t in range(tiles)], axis=1)
                product = lax.dot_general(
                    left, right, (((1,), (1,)), ((), ())), preferred_element_type=jnp.float32
                )
                totals[p] = product if totals[p] is None else totals[p] + product
        for m in range(count):
            block = totals[m // 2][:, m % 2 * width : (m % 2 + 1) * width]
            value = block[:half] + swapped(block[half:], 1.0, -1.0)
            for r in range(spaces):
                sum_ref[r, s, m] = value[r * rows : (r + 1) * rows]


def given_kernel(place_hbm, mom_hbm, x_hbm, out_ref, table_ref, turned_ref, *scratch):
    x_ref, place_ref, mom_ref, phased_ref, sum_ref, sems = scratch
    _, _, sites, width = x_ref.shape
    spaces, _, count, _, _ = out_ref.shape
    moms = mom_ref.shape[1]
    spins = moms // count
    x_copy = pltpu.make_async_copy(x_hbm, x_ref, sems.at[0])
    mom_copy = pltpu.make_async_copy(mom_hbm, mom_ref, sems.at[1])
    place_copy = pltpu.make_async_copy(place_hbm, place_ref, sems.at[2])
    mom_copy.start()
    place_copy.start()
    x_copy.start()
    row = lax.broadcasted_iota(jnp.int32, (moms, sites), 0)
    site = lax.broadcasted_iota(jnp.int32, (moms, sites), 1)
    place_copy.wait()
    space = place_ref[0]
    spin = place_ref[1]
    site = site + (space * spins + spin) * sites
    coords = (site % LAT, site // LAT % LAT, site // (LAT * LAT))
    mom_copy.wait()
    wave = jnp.zeros((moms, sites), jnp.int32)
    for d in range(3):
        value = jnp.zeros((moms, sites), jnp.int32)
        for m in range(moms):
            value = jnp.where(
                row == m, mom_ref[d, lax.rem(spin + m // count, spins) * count + m % count], value
            )
        wave = wave + value * coords[d]
    angle = (wave & (LAT - 1)).astype(jnp.float32) * (TURN / LAT)
    table_ref[0] = jnp.cos(angle)
    table_ref[1] = jnp.sin(angle)
    x_copy.wait()

    def lefts(s, c, t):
        value = x_ref[s, c, t * width : (t + 1) * width].T
        turned_ref[s, c, t] = value
        return value

    turn_and_sum(lefts, table_ref, count, phased_ref, sum_ref)
    for j in range(spaces):
        out_ref[j] = sum_ref[lax.rem(space + j, spaces)]


def given(place, mom_t, x, spaces, spins):
    slots, colours, sites, width = x.shape
    moms = mom_t.shape[1]
    count = moms // spins
    shape = (spaces, slots, count, width // 2 // spaces, width)
    tiles = sites // width
    return pl.pallas_call(
        given_kernel,
        out_shape=[
            jax.ShapeDtypeStruct(shape, jnp.float32),
            jax.ShapeDtypeStruct((2, moms, sites), jnp.float32),
            jax.ShapeDtypeStruct((slots, colours, tiles, width, width), x.dtype),
        ],
        in_specs=[ANY, ANY, ANY],
        out_specs=[VMEM] * 3,
        scratch_shapes=[
            pltpu.VMEM(x.shape, x.dtype),
            pltpu.SMEM(place.shape, jnp.int32),
            pltpu.SMEM(mom_t.shape, jnp.int32),
            pltpu.VMEM((slots, colours, count // 2, tiles, 2 * width, width), jnp.bfloat16),
            pltpu.VMEM(shape, jnp.float32),
            pltpu.SemaphoreType.DMA((3,)),
        ],
        compiler_params=params(20),
        name="given",
    )(place, in_hbm(mom_t), in_hbm(x))


def kept_kernel(place_hbm, table_ref, turned_ref, out_ref, place_ref, phased_ref, sum_ref, sem):
    spaces = out_ref.shape[0]
    place_copy = pltpu.make_async_copy(place_hbm, place_ref, sem)
    place_copy.start()
    turn_and_sum(lambda s, c, t: turned_ref[s, c, t], table_ref, 0, phased_ref, sum_ref)
    place_copy.wait()
    for j in range(spaces):
        out_ref[j] = sum_ref[lax.rem(place_ref[0] + j, spaces)]


def kept(place, table, turned, spaces, spins):
    slots, colours, tiles, width, _ = turned.shape
    count = table.shape[1] // spins
    shape = (spaces, slots, count, width // 2 // spaces, width)
    return pl.pallas_call(
        kept_kernel,
        out_shape=jax.ShapeDtypeStruct(shape, jnp.float32),
        in_specs=[ANY, VMEM, VMEM],
        out_specs=VMEM,
        scratch_shapes=[
            pltpu.SMEM(place.shape, jnp.int32),
            pltpu.VMEM((slots, colours, count // 2, tiles, 2 * width, width), jnp.bfloat16),
            pltpu.VMEM(shape, jnp.float32),
            pltpu.SemaphoreType.DMA,
        ],
        compiler_params=params(20),
        name="kept",
    )(place, table, turned)


def doubled_kernel(tau_ref, out_ref):
    pairs, vectors, wide = tau_ref.shape
    width = 2 * vectors
    for k in range(pairs):
        out_ref[k, :vectors] = tau_ref[k]
        for g in range(wide // width):
            at = slice(g * width, (g + 1) * width)
            out_ref[k, vectors:, at] = swapped(tau_ref[k, :, at], -1.0, 1.0).astype(jnp.bfloat16)


def doubled(perambulators):
    pairs, vectors, wide = perambulators.shape
    return pl.pallas_call(
        doubled_kernel,
        out_shape=jax.ShapeDtypeStruct((pairs, 2 * vectors, wide), perambulators.dtype),
        in_specs=[VMEM],
        out_specs=VMEM,
        compiler_params=params(8),
        name="doubled",
    )(perambulators)


def halfway_kernel(right_ref, *rest):
    sinks, out_ref, turn_ref = rest[:-2], rest[-2], rest[-1]
    pairs, count, rows, width = sinks[0].shape
    lines = len(sinks) * count * rows

    def step(k, carry):
        left = jnp.concatenate([sink[k].reshape(count * rows, width) for sink in sinks], axis=0)
        product = jnp.dot(left, right_ref[k], preferred_element_type=jnp.float32)
        for g in range(SPINS):
            turn_ref[pl.ds(g, lines, stride=SPINS), :] = product[:, g * width : (g + 1) * width]
        out_ref[k] = turn_ref[...].astype(jnp.bfloat16)
        return carry

    lax.fori_loop(0, pairs, step, 0)


def halfway(right, sinks):
    pairs, count, rows, width = sinks[0].shape
    lines = len(sinks) * count * rows * SPINS
    return pl.pallas_call(
        halfway_kernel,
        out_shape=jax.ShapeDtypeStruct((pairs, lines, width), jnp.bfloat16),
        in_specs=[VMEM] * (1 + len(sinks)),
        out_specs=VMEM,
        scratch_shapes=[pltpu.VMEM((lines, width), jnp.float32)],
        compiler_params=params(8),
        name="halfway",
    )(right, *sinks)


def loops_kernel(place_ref, half_ref, *rest, spaces, spins, back):
    sources = rest[:spaces]
    out_hbm, stage_ref, sem = rest[-3:]
    pairs, part, rows, spinors, width = stage_ref.shape
    block = sources[0].shape[2]
    count = rows * spinors
    where = jnp.broadcast_to(place_ref[:1, :], (block, width))
    here = [where == space for space in range(spaces)]
    owner = lax.rem(place_ref[1, 0] + spins - back, spins)
    zeros = jnp.zeros((width, width), jnp.bfloat16)
    for k in range(pairs):
        for m in range(0, part, 2):
            rights = []
            for i in range(2):
                blocks = [source[k, m + i].astype(jnp.float32) for source in sources]
                ordered = []
                for r in range(spaces):
                    value = blocks[0]
                    for j in range(1, spaces):
                        value = jnp.where(here[(r + j) % spaces], blocks[j], value)
                    ordered.append(value)
                source = jnp.concatenate(ordered, axis=0)
                turned = swapped(source, -1.0, 1.0)
                rights.append(jnp.concatenate([source, turned], axis=0).astype(jnp.bfloat16))
            right = jnp.concatenate(
                [
                    jnp.concatenate([rights[0], zeros], axis=1),
                    jnp.concatenate([zeros, rights[1]], axis=1),
                ],
                axis=0,
            )
            first = (back * part + m) * count
            left = jnp.concatenate(
                [half_ref[k, first + i * count : first + (i + 1) * count] for i in range(2)], axis=1
            )
            product = lax.dot_general(
                left, right, (((1,), (1,)), ((), ())), preferred_element_type=jnp.float32
            ).astype(jnp.bfloat16)
            for i in range(2):
                stage_ref[k, m + i] = product[:, i * width : (i + 1) * width].reshape(
                    rows, spinors, width
                )
            pltpu.make_async_copy(
                stage_ref.at[k, pl.ds(m, 2)], out_hbm.at[k, pl.ds(owner * part + m, 2)], sem
            ).start()
    pltpu.make_async_copy(stage_ref, out_hbm.at[:, pl.ds(owner * part, part)], sem).wait()


def loops(place_rows, half, sources, back, spins, before):
    pairs, lines, width = half.shape
    spaces = len(sources)
    _, part, _, _ = sources[0].shape
    rows = lines // (spins * part * SPINS)
    operands = [place_rows, half, *sources] + ([] if before is None else [before])
    return pl.pallas_call(
        functools.partial(loops_kernel, spaces=spaces, spins=spins, back=back),
        out_shape=jax.ShapeDtypeStruct((pairs, spins * part, rows, SPINS, width), jnp.bfloat16),
        in_specs=[VMEM] * (2 + spaces) + ([] if before is None else [HBM]),
        out_specs=HBM,
        scratch_shapes=[
            pltpu.VMEM((pairs, part, rows, SPINS, width), jnp.bfloat16),
            pltpu.SemaphoreType.DMA,
        ],
        input_output_aliases={} if before is None else {2 + spaces: 0},
        compiler_params=params(16),
    )(*operands)


def shifted(value, axis, by):
    size = lax.axis_size(axis)
    return lax.ppermute(value, axis, [(i, (i + by) % size) for i in range(size)])


def around(value, axis):
    parts = [value]
    for j in range(1, lax.axis_size(axis)):
        parts.append(shifted(value, axis, j))
    return parts


def targets(size):
    ring = [0, *range(1, size, 2), *reversed(range(2, size, 2))]
    place = {member: n for n, member in enumerate(ring)}
    return [[ring[(place[i] + j) % size] for i in range(size)] for j in range(1, size)]


def exchanged(value, axis):
    parts = [value]
    for to in targets(lax.axis_size(axis)):
        parts.append(lax.ppermute(value, axis, list(enumerate(to))))
    return parts


def arrivals(size):
    table = [[0] * size for _ in range(size)]
    for n, to in enumerate(targets(size)):
        for sender, receiver in enumerate(to):
            table[receiver][sender] = n + 1
    return table


def selected(index, candidates):
    flag = index[:, None, None, None]
    result = jnp.broadcast_to(candidates[0], (index.shape[0],) + candidates[0].shape)
    for n in range(1, len(candidates)):
        result = jnp.where(flag == n, candidates[n], result)
    return result


def per_device(eigenvectors, momenta, time_pairs, slot_map, perambulators):
    spaces = lax.axis_size("space")
    spins = lax.axis_size("spin")
    slots = eigenvectors.shape[0]
    place = jnp.stack([lax.axis_index("space"), lax.axis_index("spin")]).astype(jnp.int32)
    place_rows = jnp.broadcast_to(place[:, None], (2, 2 * perambulators.shape[1]))
    times = slot_map.shape[0]
    named = time_pairs[:, :, None] == lax.iota(jnp.int32, times)
    slot = jnp.sum(jnp.where(named, slot_map, 0), axis=-1)
    members = lax.axis_size("tm")
    table = jnp.array(arrivals(members), jnp.int32)
    row = jnp.sum(
        jnp.where((lax.iota(jnp.int32, members) == lax.axis_index("tm"))[:, None], table, 0), 0
    )
    held = (slot // slots)[..., None] == lax.iota(jnp.int32, members)
    index = jnp.sum(jnp.where(held, row, 0), axis=-1) * slots + slot % slots

    spin = lax.axis_index("spin")
    x = jnp.transpose(eigenvectors, (0, 2, 1, 3))
    send, table, turned = given(place, momenta.T, x, spaces, spins)
    received = shifted(send, "spin", 1)
    total = kept(place, table, turned, spaces, spins)
    total = total + received
    row_share = total[0]
    for j in range(1, spaces):
        value = shifted(total[j].astype(jnp.bfloat16), "space", j)
        row_share = row_share + value.astype(jnp.float32)
    row_share = row_share.astype(jnp.bfloat16)
    arrived = exchanged(row_share, "tm")
    candidates = [value[s] for value in arrived for s in range(slots)]
    source_share = selected(index[:, 1], candidates)
    sink_share = selected(index[:, 0], candidates)
    rows = sink_share.shape[2] // spins
    sinks = []
    for i in range(spins):
        block = lax.dynamic_slice_in_dim(sink_share, (spin + i) % spins * rows, rows, axis=2)
        if i:
            block = shifted(block, "spin", i)
        sinks.append(block)
    right = doubled(perambulators)
    half = halfway(right, sinks)
    far = around(source_share, "space")
    near = [around(value, "spin") for value in far]
    result = None
    for back in range(spins):
        sources = [group[back] for group in near]
        result = loops(place_rows, half, sources, back, spins, result)
    return result


def solution(mesh):
    placed = (
        P(("cfg", "tm"), ("space", "spin"), None, None),
        P(),
        P(("cfg", "tm"), None),
        P(),
        P(("cfg", "tm"), None, None),
    )

    return jax.shard_map(
        per_device,
        mesh=mesh,
        in_specs=placed,
        out_specs=P(("cfg", "tm"), None, ("space", "spin"), None, None),
        check_vma=False,
    )
```

```python
import functools

import jax
import jax.numpy as jnp
from jax import lax
from jax.experimental import pallas as pl
from jax.experimental.pallas import tpu as pltpu
from jax.sharding import PartitionSpec as P


LAT = 32
TURN = 6.283185307179586
SPINS = 16
SMEM = pl.BlockSpec(memory_space=pltpu.SMEM)
VMEM = pl.BlockSpec(memory_space=pltpu.VMEM)
HBM = pl.BlockSpec(memory_space=pltpu.HBM)
ANY = pl.BlockSpec(memory_space=pl.ANY)


def params(mib):
    return pltpu.CompilerParams(vmem_limit_bytes=mib * 1024 * 1024)


def in_hbm(value):
    return pltpu.with_memory_space_constraint(value, pltpu.HBM)


def swapped(value, first, second):
    half = value.shape[1] // 2
    lane = lax.broadcasted_iota(jnp.int32, value.shape, 1)
    sign = jnp.where(lane < half, first, second).astype(jnp.float32)
    return pltpu.roll(value.astype(jnp.float32), half, 1) * sign


def turn_and_sum(lefts, table_ref, first, phased_ref, sum_ref):
    slots, colours, _, tiles, _, width = phased_ref.shape
    half = width // 2
    spaces, _, count, rows, _ = sum_ref.shape
    for s in range(slots):
        totals = [None] * (count // 2)
        for c in range(colours):
            left = [lefts(s, c, t) for t in range(tiles)]
            for t in range(tiles):
                at = slice(t * width, (t + 1) * width)
                real = left[t][:half].astype(jnp.float32)
                imag = left[t][half:].astype(jnp.float32)
                for m in range(count):
                    row = slice(first + m, first + m + 1)
                    cosine = jnp.broadcast_to(table_ref[0, row, at], (half, width))
                    sine = jnp.broadcast_to(table_ref[1, row, at], (half, width))
                    top = m % 2 * width
                    phased_ref[s, c, m // 2, t, top : top + half] = (
                        cosine * real - sine * imag
                    ).astype(jnp.bfloat16)
                    phased_ref[s, c, m // 2, t, top + half : top + width] = (
                        sine * real + cosine * imag
                    ).astype(jnp.bfloat16)
            left = jnp.concatenate(left, axis=1)
            for p in range(count // 2):
                right = jnp.concatenate([phased_ref[s, c, p, t] for t in range(tiles)], axis=1)
                product = lax.dot_general(
                    left, right, (((1,), (1,)), ((), ())), preferred_element_type=jnp.float32
                )
                totals[p] = product if totals[p] is None else totals[p] + product
        for m in range(count):
            block = totals[m // 2][:, m % 2 * width : (m % 2 + 1) * width]
            value = block[:half] + swapped(block[half:], 1.0, -1.0)
            for r in range(spaces):
                sum_ref[r, s, m] = value[r * rows : (r + 1) * rows]


def given_kernel(place_hbm, mom_hbm, x_hbm, out_ref, table_ref, turned_ref, *scratch):
    x_ref, place_ref, mom_ref, phased_ref, sum_ref, sems = scratch
    _, _, sites, width = x_ref.shape
    spaces, _, count, _, _ = out_ref.shape
    moms = mom_ref.shape[1]
    spins = moms // count
    x_copy = pltpu.make_async_copy(x_hbm, x_ref, sems.at[0])
    mom_copy = pltpu.make_async_copy(mom_hbm, mom_ref, sems.at[1])
    place_copy = pltpu.make_async_copy(place_hbm, place_ref, sems.at[2])
    mom_copy.start()
    place_copy.start()
    x_copy.start()
    row = lax.broadcasted_iota(jnp.int32, (moms, sites), 0)
    site = lax.broadcasted_iota(jnp.int32, (moms, sites), 1)
    place_copy.wait()
    space = place_ref[0]
    spin = place_ref[1]
    site = site + (space * spins + spin) * sites
    coords = (site % LAT, site // LAT % LAT, site // (LAT * LAT))
    mom_copy.wait()
    wave = jnp.zeros((moms, sites), jnp.int32)
    for d in range(3):
        value = jnp.zeros((moms, sites), jnp.int32)
        for m in range(moms):
            value = jnp.where(
                row == m, mom_ref[d, lax.rem(spin + m // count, spins) * count + m % count], value
            )
        wave = wave + value * coords[d]
    angle = (wave & (LAT - 1)).astype(jnp.float32) * (TURN / LAT)
    table_ref[0] = jnp.cos(angle)
    table_ref[1] = jnp.sin(angle)
    x_copy.wait()

    def lefts(s, c, t):
        value = x_ref[s, c, t * width : (t + 1) * width].T
        turned_ref[s, c, t] = value
        return value

    turn_and_sum(lefts, table_ref, count, phased_ref, sum_ref)
    for j in range(spaces):
        out_ref[j] = sum_ref[lax.rem(space + j, spaces)]


def given(place, mom_t, x, spaces, spins):
    slots, colours, sites, width = x.shape
    moms = mom_t.shape[1]
    count = moms // spins
    shape = (spaces, slots, count, width // 2 // spaces, width)
    tiles = sites // width
    return pl.pallas_call(
        given_kernel,
        out_shape=[
            jax.ShapeDtypeStruct(shape, jnp.float32),
            jax.ShapeDtypeStruct((2, moms, sites), jnp.float32),
            jax.ShapeDtypeStruct((slots, colours, tiles, width, width), x.dtype),
        ],
        in_specs=[ANY, ANY, ANY],
        out_specs=[VMEM] * 3,
        scratch_shapes=[
            pltpu.VMEM(x.shape, x.dtype),
            pltpu.SMEM(place.shape, jnp.int32),
            pltpu.SMEM(mom_t.shape, jnp.int32),
            pltpu.VMEM((slots, colours, count // 2, tiles, 2 * width, width), jnp.bfloat16),
            pltpu.VMEM(shape, jnp.float32),
            pltpu.SemaphoreType.DMA((3,)),
        ],
        compiler_params=params(20),
        name="given",
    )(place, in_hbm(mom_t), in_hbm(x))


def kept_kernel(place_hbm, table_ref, turned_ref, out_ref, place_ref, phased_ref, sum_ref, sem):
    spaces = out_ref.shape[0]
    place_copy = pltpu.make_async_copy(place_hbm, place_ref, sem)
    place_copy.start()
    turn_and_sum(lambda s, c, t: turned_ref[s, c, t], table_ref, 0, phased_ref, sum_ref)
    place_copy.wait()
    for j in range(spaces):
        out_ref[j] = sum_ref[lax.rem(place_ref[0] + j, spaces)]


def kept(place, table, turned, spaces, spins):
    slots, colours, tiles, width, _ = turned.shape
    count = table.shape[1] // spins
    shape = (spaces, slots, count, width // 2 // spaces, width)
    return pl.pallas_call(
        kept_kernel,
        out_shape=jax.ShapeDtypeStruct(shape, jnp.float32),
        in_specs=[ANY, VMEM, VMEM],
        out_specs=VMEM,
        scratch_shapes=[
            pltpu.SMEM(place.shape, jnp.int32),
            pltpu.VMEM((slots, colours, count // 2, tiles, 2 * width, width), jnp.bfloat16),
            pltpu.VMEM(shape, jnp.float32),
            pltpu.SemaphoreType.DMA,
        ],
        compiler_params=params(20),
        name="kept",
    )(place, table, turned)


def doubled_kernel(tau_ref, out_ref):
    pairs, vectors, wide = tau_ref.shape
    width = 2 * vectors
    for k in range(pairs):
        out_ref[k, :vectors] = tau_ref[k]
        for g in range(wide // width):
            at = slice(g * width, (g + 1) * width)
            out_ref[k, vectors:, at] = swapped(tau_ref[k, :, at], -1.0, 1.0).astype(jnp.bfloat16)


def doubled(perambulators):
    pairs, vectors, wide = perambulators.shape
    return pl.pallas_call(
        doubled_kernel,
        out_shape=jax.ShapeDtypeStruct((pairs, 2 * vectors, wide), perambulators.dtype),
        in_specs=[VMEM],
        out_specs=VMEM,
        compiler_params=params(8),
        name="doubled",
    )(perambulators)


def halfway_kernel(right_ref, *rest):
    sinks, out_ref, turn_ref = rest[:-2], rest[-2], rest[-1]
    pairs, count, rows, width = sinks[0].shape
    lines = len(sinks) * count * rows

    def step(k, carry):
        left = jnp.concatenate([sink[k].reshape(count * rows, width) for sink in sinks], axis=0)
        product = jnp.dot(left, right_ref[k], preferred_element_type=jnp.float32)
        for g in range(SPINS):
            turn_ref[pl.ds(g, lines, stride=SPINS + 1), :] = product[
                :, g * width : (g + 1) * width
            ]
        for n in range(lines):
            out_ref[k, n * SPINS : (n + 1) * SPINS] = turn_ref[
                n * (SPINS + 1) : n * (SPINS + 1) + SPINS
            ].astype(jnp.bfloat16)
        return carry

    lax.fori_loop(0, pairs, step, 0)


def halfway(right, sinks):
    pairs, count, rows, width = sinks[0].shape
    lines = len(sinks) * count * rows * SPINS
    return pl.pallas_call(
        halfway_kernel,
        out_shape=jax.ShapeDtypeStruct((pairs, lines, width), jnp.bfloat16),
        in_specs=[VMEM] * (1 + len(sinks)),
        out_specs=VMEM,
        scratch_shapes=[pltpu.VMEM((lines // SPINS * (SPINS + 1) + SPINS, width), jnp.float32)],
        compiler_params=params(8),
        name="halfway",
    )(right, *sinks)


def loops_kernel(place_ref, half_ref, *rest, spaces, spins, back):
    sources = rest[:spaces]
    out_hbm, stage_ref, sem = rest[-3:]
    pairs, part, rows, spinors, width = stage_ref.shape
    block = sources[0].shape[2]
    count = rows * spinors
    where = jnp.broadcast_to(place_ref[:1, :], (block, width))
    here = [where == space for space in range(spaces)]
    owner = lax.rem(place_ref[1, 0] + spins - back, spins)
    zeros = jnp.zeros((width, width), jnp.bfloat16)
    for k in range(pairs):
        for m in range(0, part, 2):
            rights = []
            for i in range(2):
                blocks = [source[k, m + i].astype(jnp.float32) for source in sources]
                ordered = []
                for r in range(spaces):
                    value = blocks[0]
                    for j in range(1, spaces):
                        value = jnp.where(here[(r + j) % spaces], blocks[j], value)
                    ordered.append(value)
                source = jnp.concatenate(ordered, axis=0)
                turned = swapped(source, -1.0, 1.0)
                rights.append(jnp.concatenate([source, turned], axis=0).astype(jnp.bfloat16))
            right = jnp.concatenate(
                [
                    jnp.concatenate([rights[0], zeros], axis=1),
                    jnp.concatenate([zeros, rights[1]], axis=1),
                ],
                axis=0,
            )
            first = (back * part + m) * count
            left = jnp.concatenate(
                [half_ref[k, first + i * count : first + (i + 1) * count] for i in range(2)], axis=1
            )
            product = lax.dot_general(
                left, right, (((1,), (1,)), ((), ())), preferred_element_type=jnp.float32
            ).astype(jnp.bfloat16)
            for i in range(2):
                stage_ref[k, m + i] = product[:, i * width : (i + 1) * width].reshape(
                    rows, spinors, width
                )
            pltpu.make_async_copy(
                stage_ref.at[k, pl.ds(m, 2)], out_hbm.at[k, pl.ds(owner * part + m, 2)], sem
            ).start()
    pltpu.make_async_copy(stage_ref, out_hbm.at[:, pl.ds(owner * part, part)], sem).wait()


def loops(place_rows, half, sources, back, spins, before):
    pairs, lines, width = half.shape
    spaces = len(sources)
    _, part, _, _ = sources[0].shape
    rows = lines // (spins * part * SPINS)
    operands = [place_rows, half, *sources] + ([] if before is None else [before])
    return pl.pallas_call(
        functools.partial(loops_kernel, spaces=spaces, spins=spins, back=back),
        out_shape=jax.ShapeDtypeStruct((pairs, spins * part, rows, SPINS, width), jnp.bfloat16),
        in_specs=[VMEM] * (2 + spaces) + ([] if before is None else [HBM]),
        out_specs=HBM,
        scratch_shapes=[
            pltpu.VMEM((pairs, part, rows, SPINS, width), jnp.bfloat16),
            pltpu.SemaphoreType.DMA,
        ],
        input_output_aliases={} if before is None else {2 + spaces: 0},
        compiler_params=params(16),
    )(*operands)


def shifted(value, axis, by):
    size = lax.axis_size(axis)
    return lax.ppermute(value, axis, [(i, (i + by) % size) for i in range(size)])


def around(value, axis):
    parts = [value]
    for j in range(1, lax.axis_size(axis)):
        parts.append(shifted(value, axis, j))
    return parts


def targets(size):
    ring = [0, *range(1, size, 2), *reversed(range(2, size, 2))]
    place = {member: n for n, member in enumerate(ring)}
    return [[ring[(place[i] + j) % size] for i in range(size)] for j in range(1, size)]


def exchanged(value, axis):
    parts = [value]
    for to in targets(lax.axis_size(axis)):
        parts.append(lax.ppermute(value, axis, list(enumerate(to))))
    return parts


def arrivals(size):
    table = [[0] * size for _ in range(size)]
    for n, to in enumerate(targets(size)):
        for sender, receiver in enumerate(to):
            table[receiver][sender] = n + 1
    return table


def selected(index, candidates):
    flag = index[:, None, None, None]
    result = jnp.broadcast_to(candidates[0], (index.shape[0],) + candidates[0].shape)
    for n in range(1, len(candidates)):
        result = jnp.where(flag == n, candidates[n], result)
    return result


def per_device(eigenvectors, momenta, time_pairs, slot_map, perambulators):
    spaces = lax.axis_size("space")
    spins = lax.axis_size("spin")
    slots = eigenvectors.shape[0]
    place = jnp.stack([lax.axis_index("space"), lax.axis_index("spin")]).astype(jnp.int32)
    place_rows = jnp.broadcast_to(place[:, None], (2, 2 * perambulators.shape[1]))
    times = slot_map.shape[0]
    named = time_pairs[:, :, None] == lax.iota(jnp.int32, times)
    slot = jnp.sum(jnp.where(named, slot_map, 0), axis=-1)
    members = lax.axis_size("tm")
    table = jnp.array(arrivals(members), jnp.int32)
    row = jnp.sum(
        jnp.where((lax.iota(jnp.int32, members) == lax.axis_index("tm"))[:, None], table, 0), 0
    )
    held = (slot // slots)[..., None] == lax.iota(jnp.int32, members)
    index = jnp.sum(jnp.where(held, row, 0), axis=-1) * slots + slot % slots

    spin = lax.axis_index("spin")
    x = jnp.transpose(eigenvectors, (0, 2, 1, 3))
    send, table, turned = given(place, momenta.T, x, spaces, spins)
    received = shifted(send, "spin", 1)
    total = kept(place, table, turned, spaces, spins)
    total = total + received
    row_share = total[0]
    for j in range(1, spaces):
        value = shifted(total[j].astype(jnp.bfloat16), "space", j)
        row_share = row_share + value.astype(jnp.float32)
    row_share = row_share.astype(jnp.bfloat16)
    arrived = exchanged(row_share, "tm")
    candidates = [value[s] for value in arrived for s in range(slots)]
    source_share = selected(index[:, 1], candidates)
    sink_share = selected(index[:, 0], candidates)
    rows = sink_share.shape[2] // spins
    sinks = []
    for i in range(spins):
        block = lax.dynamic_slice_in_dim(sink_share, (spin + i) % spins * rows, rows, axis=2)
        if i:
            block = shifted(block, "spin", i)
        sinks.append(block)
    right = doubled(perambulators)
    half = halfway(right, sinks)
    far = around(source_share, "space")
    near = [around(value, "spin") for value in far]
    result = None
    for back in range(spins):
        sources = [group[back] for group in near]
        result = loops(place_rows, half, sources, back, spins, result)
    return result


def solution(mesh):
    placed = (
        P(("cfg", "tm"), ("space", "spin"), None, None),
        P(),
        P(("cfg", "tm"), None),
        P(),
        P(("cfg", "tm"), None, None),
    )

    return jax.shard_map(
        per_device,
        mesh=mesh,
        in_specs=placed,
        out_specs=P(("cfg", "tm"), None, ("space", "spin"), None, None),
        check_vma=False,
    )
```

```python
import functools

import jax
import jax.numpy as jnp
from jax import lax
from jax.experimental import pallas as pl
from jax.experimental.pallas import tpu as pltpu
from jax.sharding import PartitionSpec as P


LAT = 32
TURN = 6.283185307179586
SPINS = 16
SMEM = pl.BlockSpec(memory_space=pltpu.SMEM)
VMEM = pl.BlockSpec(memory_space=pltpu.VMEM)
HBM = pl.BlockSpec(memory_space=pltpu.HBM)
ANY = pl.BlockSpec(memory_space=pl.ANY)


def params(mib):
    return pltpu.CompilerParams(vmem_limit_bytes=mib * 1024 * 1024)


def in_hbm(value):
    return pltpu.with_memory_space_constraint(value, pltpu.HBM)


def swapped(value, first, second):
    half = value.shape[1] // 2
    lane = lax.broadcasted_iota(jnp.int32, value.shape, 1)
    sign = jnp.where(lane < half, first, second).astype(jnp.float32)
    return pltpu.roll(value.astype(jnp.float32), half, 1) * sign


def turn_and_sum(lefts, table_ref, first, phased_ref, sum_ref):
    slots, colours, _, tiles, _, width = phased_ref.shape
    half = width // 2
    spaces, _, count, rows, _ = sum_ref.shape
    for s in range(slots):
        totals = [None] * (count // 2)
        for c in range(colours):
            left = [lefts(s, c, t) for t in range(tiles)]
            for t in range(tiles):
                at = slice(t * width, (t + 1) * width)
                real = left[t][:half].astype(jnp.float32)
                imag = left[t][half:].astype(jnp.float32)
                for m in range(count):
                    row = slice(first + m, first + m + 1)
                    cosine = jnp.broadcast_to(table_ref[0, row, at], (half, width))
                    sine = jnp.broadcast_to(table_ref[1, row, at], (half, width))
                    top = m % 2 * width
                    phased_ref[s, c, m // 2, t, top : top + half] = (
                        cosine * real - sine * imag
                    ).astype(jnp.bfloat16)
                    phased_ref[s, c, m // 2, t, top + half : top + width] = (
                        sine * real + cosine * imag
                    ).astype(jnp.bfloat16)
            left = jnp.concatenate(left, axis=1)
            for p in range(count // 2):
                right = jnp.concatenate([phased_ref[s, c, p, t] for t in range(tiles)], axis=1)
                product = lax.dot_general(
                    left, right, (((1,), (1,)), ((), ())), preferred_element_type=jnp.float32
                )
                totals[p] = product if totals[p] is None else totals[p] + product
        for m in range(count):
            block = totals[m // 2][:, m % 2 * width : (m % 2 + 1) * width]
            value = block[:half] + swapped(block[half:], 1.0, -1.0)
            for r in range(spaces):
                sum_ref[r, s, m] = value[r * rows : (r + 1) * rows]


def given_kernel(place_hbm, mom_hbm, x_hbm, out_ref, table_ref, turned_ref, *scratch):
    x_ref, place_ref, mom_ref, phased_ref, sum_ref, sems = scratch
    _, _, sites, width = x_ref.shape
    spaces, _, count, _, _ = out_ref.shape
    moms = mom_ref.shape[1]
    spins = moms // count
    x_copy = pltpu.make_async_copy(x_hbm, x_ref, sems.at[0])
    mom_copy = pltpu.make_async_copy(mom_hbm, mom_ref, sems.at[1])
    place_copy = pltpu.make_async_copy(place_hbm, place_ref, sems.at[2])
    mom_copy.start()
    place_copy.start()
    x_copy.start()
    row = lax.broadcasted_iota(jnp.int32, (moms, sites), 0)
    site = lax.broadcasted_iota(jnp.int32, (moms, sites), 1)
    place_copy.wait()
    space = place_ref[0]
    spin = place_ref[1]
    site = site + (space * spins + spin) * sites
    coords = (site % LAT, site // LAT % LAT, site // (LAT * LAT))
    mom_copy.wait()
    wave = jnp.zeros((moms, sites), jnp.int32)
    for d in range(3):
        value = jnp.zeros((moms, sites), jnp.int32)
        for m in range(moms):
            value = jnp.where(
                row == m, mom_ref[d, lax.rem(spin + m // count, spins) * count + m % count], value
            )
        wave = wave + value * coords[d]
    angle = (wave & (LAT - 1)).astype(jnp.float32) * (TURN / LAT)
    table_ref[0] = jnp.cos(angle)
    table_ref[1] = jnp.sin(angle)
    x_copy.wait()

    def lefts(s, c, t):
        value = x_ref[s, c, t * width : (t + 1) * width].T
        turned_ref[s, c, t] = value
        return value

    turn_and_sum(lefts, table_ref, count, phased_ref, sum_ref)
    for j in range(spaces):
        out_ref[j] = sum_ref[lax.rem(space + j, spaces)]


def given(place, mom_t, x, spaces, spins):
    slots, colours, sites, width = x.shape
    moms = mom_t.shape[1]
    count = moms // spins
    shape = (spaces, slots, count, width // 2 // spaces, width)
    tiles = sites // width
    return pl.pallas_call(
        given_kernel,
        out_shape=[
            jax.ShapeDtypeStruct(shape, jnp.float32),
            jax.ShapeDtypeStruct((2, moms, sites), jnp.float32),
            jax.ShapeDtypeStruct((slots, colours, tiles, width, width), x.dtype),
        ],
        in_specs=[ANY, ANY, ANY],
        out_specs=[VMEM] * 3,
        scratch_shapes=[
            pltpu.VMEM(x.shape, x.dtype),
            pltpu.SMEM(place.shape, jnp.int32),
            pltpu.SMEM(mom_t.shape, jnp.int32),
            pltpu.VMEM((slots, colours, count // 2, tiles, 2 * width, width), jnp.bfloat16),
            pltpu.VMEM(shape, jnp.float32),
            pltpu.SemaphoreType.DMA((3,)),
        ],
        compiler_params=params(20),
        name="given",
    )(place, in_hbm(mom_t), in_hbm(x))


def kept_kernel(place_hbm, table_ref, turned_ref, out_ref, place_ref, phased_ref, sum_ref, sem):
    spaces = out_ref.shape[0]
    place_copy = pltpu.make_async_copy(place_hbm, place_ref, sem)
    place_copy.start()
    turn_and_sum(lambda s, c, t: turned_ref[s, c, t], table_ref, 0, phased_ref, sum_ref)
    place_copy.wait()
    for j in range(spaces):
        out_ref[j] = sum_ref[lax.rem(place_ref[0] + j, spaces)]


def kept(place, table, turned, spaces, spins):
    slots, colours, tiles, width, _ = turned.shape
    count = table.shape[1] // spins
    shape = (spaces, slots, count, width // 2 // spaces, width)
    return pl.pallas_call(
        kept_kernel,
        out_shape=jax.ShapeDtypeStruct(shape, jnp.float32),
        in_specs=[ANY, VMEM, VMEM],
        out_specs=VMEM,
        scratch_shapes=[
            pltpu.SMEM(place.shape, jnp.int32),
            pltpu.VMEM((slots, colours, count // 2, tiles, 2 * width, width), jnp.bfloat16),
            pltpu.VMEM(shape, jnp.float32),
            pltpu.SemaphoreType.DMA,
        ],
        compiler_params=params(20),
        name="kept",
    )(place, table, turned)


def doubled_kernel(tau_ref, out_ref):
    pairs, vectors, wide = tau_ref.shape
    width = 2 * vectors
    for k in range(pairs):
        out_ref[k, :vectors] = tau_ref[k]
        for g in range(wide // width):
            at = slice(g * width, (g + 1) * width)
            out_ref[k, vectors:, at] = swapped(tau_ref[k, :, at], -1.0, 1.0).astype(jnp.bfloat16)


def doubled(perambulators):
    pairs, vectors, wide = perambulators.shape
    return pl.pallas_call(
        doubled_kernel,
        out_shape=jax.ShapeDtypeStruct((pairs, 2 * vectors, wide), perambulators.dtype),
        in_specs=[VMEM],
        out_specs=VMEM,
        compiler_params=params(8),
        name="doubled",
    )(perambulators)


def halfway_kernel(right_ref, *rest):
    sinks, out_ref, turn_ref = rest[:-2], rest[-2], rest[-1]
    pairs, count, rows, width = sinks[0].shape
    lines = len(sinks) * count * rows

    def step(k, carry):
        left = jnp.concatenate([sink[k].reshape(count * rows, width) for sink in sinks], axis=0)
        product = jnp.dot(left, right_ref[k], preferred_element_type=jnp.float32)
        for g in range(SPINS):
            turn_ref[pl.ds(g, lines, stride=SPINS + 1), :] = product[
                :, g * width : (g + 1) * width
            ]
        for n in range(lines):
            out_ref[k, n * SPINS : (n + 1) * SPINS] = turn_ref[
                n * (SPINS + 1) : n * (SPINS + 1) + SPINS
            ].astype(jnp.bfloat16)
        return carry

    lax.fori_loop(0, pairs, step, 0)


def halfway(right, sinks):
    pairs, count, rows, width = sinks[0].shape
    lines = len(sinks) * count * rows * SPINS
    return pl.pallas_call(
        halfway_kernel,
        out_shape=jax.ShapeDtypeStruct((pairs, lines, width), jnp.bfloat16),
        in_specs=[VMEM] * (1 + len(sinks)),
        out_specs=VMEM,
        scratch_shapes=[pltpu.VMEM((lines // SPINS * (SPINS + 1) + SPINS, width), jnp.float32)],
        compiler_params=params(8),
        name="halfway",
    )(right, *sinks)


def loops_kernel(place_ref, half_ref, *rest, spaces, spins, back):
    sources = rest[:spaces]
    out_hbm, stage_ref, sem = rest[-3:]
    pairs, part, rows, spinors, width = stage_ref.shape
    block = sources[0].shape[2]
    count = rows * spinors
    where = jnp.broadcast_to(place_ref[:1, :], (block, width))
    here = [where == space for space in range(spaces)]
    owner = lax.rem(place_ref[1, 0] + spins - back, spins)
    zeros = jnp.zeros((width, width), jnp.bfloat16)
    for k in range(pairs):
        for m in range(0, part, 2):
            rights = []
            for i in range(2):
                blocks = [source[k, m + i].astype(jnp.float32) for source in sources]
                ordered = []
                for r in range(spaces):
                    value = blocks[0]
                    for j in range(1, spaces):
                        value = jnp.where(here[(r + j) % spaces], blocks[j], value)
                    ordered.append(value)
                source = jnp.concatenate(ordered, axis=0)
                turned = swapped(source, -1.0, 1.0)
                rights.append(jnp.concatenate([source, turned], axis=0).astype(jnp.bfloat16))
            right = jnp.concatenate(
                [
                    jnp.concatenate([rights[0], zeros], axis=1),
                    jnp.concatenate([zeros, rights[1]], axis=1),
                ],
                axis=0,
            )
            first = (back * part + m) * count
            left = jnp.concatenate(
                [half_ref[k, first + i * count : first + (i + 1) * count] for i in range(2)], axis=1
            )
            product = lax.dot_general(
                left, right, (((1,), (1,)), ((), ())), preferred_element_type=jnp.float32
            ).astype(jnp.bfloat16)
            for i in range(2):
                stage_ref[k, m + i] = product[:, i * width : (i + 1) * width].reshape(
                    rows, spinors, width
                )
            pltpu.make_async_copy(
                stage_ref.at[k, pl.ds(m, 2)], out_hbm.at[k, pl.ds(owner * part + m, 2)], sem
            ).start()
    pltpu.make_async_copy(stage_ref, out_hbm.at[:, pl.ds(owner * part, part)], sem).wait()


def loops(place_rows, half, sources, back, spins, before):
    pairs, lines, width = half.shape
    spaces = len(sources)
    _, part, _, _ = sources[0].shape
    rows = lines // (spins * part * SPINS)
    operands = [place_rows, half, *sources] + ([] if before is None else [before])
    return pl.pallas_call(
        functools.partial(loops_kernel, spaces=spaces, spins=spins, back=back),
        out_shape=jax.ShapeDtypeStruct((pairs, spins * part, rows, SPINS, width), jnp.bfloat16),
        in_specs=[VMEM] * (2 + spaces) + ([] if before is None else [HBM]),
        out_specs=HBM,
        scratch_shapes=[
            pltpu.VMEM((pairs, part, rows, SPINS, width), jnp.bfloat16),
            pltpu.SemaphoreType.DMA,
        ],
        input_output_aliases={} if before is None else {2 + spaces: 0},
        compiler_params=params(16),
    )(*operands)


def shifted(value, axis, by):
    size = lax.axis_size(axis)
    return lax.ppermute(value, axis, [(i, (i + by) % size) for i in range(size)])


def around(value, axis):
    parts = [value]
    for j in range(1, lax.axis_size(axis)):
        parts.append(shifted(value, axis, j))
    return parts


def targets(size):
    ring = [0, *range(1, size, 2), *reversed(range(2, size, 2))]
    place = {member: n for n, member in enumerate(ring)}
    return [[ring[(place[i] + j) % size] for i in range(size)] for j in range(1, size)]


def exchanged(value, axis):
    parts = [value]
    for to in targets(lax.axis_size(axis)):
        parts.append(lax.ppermute(value, axis, list(enumerate(to))))
    return parts


def arrivals(size):
    table = [[0] * size for _ in range(size)]
    for n, to in enumerate(targets(size)):
        for sender, receiver in enumerate(to):
            table[receiver][sender] = n + 1
    return table


def selected(index, candidates):
    flag = index[:, None, None, None]
    result = jnp.broadcast_to(candidates[0], (index.shape[0],) + candidates[0].shape)
    for n in range(1, len(candidates)):
        result = jnp.where(flag == n, candidates[n], result)
    return result


def per_device(eigenvectors, momenta, time_pairs, slot_map, perambulators):
    spaces = lax.axis_size("space")
    spins = lax.axis_size("spin")
    slots = eigenvectors.shape[0]
    place = jnp.stack([lax.axis_index("space"), lax.axis_index("spin")]).astype(jnp.int32)
    place_rows = jnp.broadcast_to(place[:, None], (2, 2 * perambulators.shape[1]))
    times = slot_map.shape[0]
    named = time_pairs[:, :, None] == lax.iota(jnp.int32, times)
    slot = jnp.sum(jnp.where(named, slot_map, 0), axis=-1)
    members = lax.axis_size("tm")
    table = jnp.array(arrivals(members), jnp.int32)
    row = jnp.sum(
        jnp.where((lax.iota(jnp.int32, members) == lax.axis_index("tm"))[:, None], table, 0), 0
    )
    held = (slot // slots)[..., None] == lax.iota(jnp.int32, members)
    index = jnp.sum(jnp.where(held, row, 0), axis=-1) * slots + slot % slots

    spin = lax.axis_index("spin")
    x = jnp.transpose(eigenvectors, (0, 2, 1, 3))
    send, table, turned = given(place, momenta.T, x, spaces, spins)
    received = shifted(send, "spin", 1)
    total = kept(place, table, turned, spaces, spins)
    total = total + received
    row_share = total[0]
    for j in range(1, spaces):
        value = shifted(total[j].astype(jnp.bfloat16), "space", j)
        row_share = row_share + value.astype(jnp.float32)
    row_share = row_share.astype(jnp.bfloat16)
    arrived = exchanged(row_share, "tm")
    candidates = [value[s] for value in arrived for s in range(slots)]
    early = len(candidates) - slots
    chosen = [selected(index[:, side], candidates[:early]) for side in range(2)]
    chosen = lax.optimization_barrier(chosen)
    for n in range(early, len(candidates)):
        chosen = [
            jnp.where(index[:, side, None, None, None] == n, candidates[n], chosen[side])
            for side in range(2)
        ]
    sink_share, source_share = chosen
    rows = sink_share.shape[2] // spins
    sinks = []
    for i in range(spins):
        block = lax.dynamic_slice_in_dim(sink_share, (spin + i) % spins * rows, rows, axis=2)
        if i:
            block = shifted(block, "spin", i)
        sinks.append(block)
    right = doubled(perambulators)
    half = halfway(right, sinks)
    far = around(source_share, "space")
    near = [around(value, "spin") for value in far]
    result = None
    for back in range(spins):
        sources = [group[back] for group in near]
        result = loops(place_rows, half, sources, back, spins, result)
    return result


def solution(mesh):
    placed = (
        P(("cfg", "tm"), ("space", "spin"), None, None),
        P(),
        P(("cfg", "tm"), None),
        P(),
        P(("cfg", "tm"), None, None),
    )

    return jax.shard_map(
        per_device,
        mesh=mesh,
        in_specs=placed,
        out_specs=P(("cfg", "tm"), None, ("space", "spin"), None, None),
        check_vma=False,
    )
```

```python
import functools

import jax
import jax.numpy as jnp
from jax import lax
from jax.experimental import pallas as pl
from jax.experimental.pallas import tpu as pltpu
from jax.sharding import PartitionSpec as P


LAT = 32
TURN = 6.283185307179586
SPINS = 16
SMEM = pl.BlockSpec(memory_space=pltpu.SMEM)
VMEM = pl.BlockSpec(memory_space=pltpu.VMEM)
HBM = pl.BlockSpec(memory_space=pltpu.HBM)
ANY = pl.BlockSpec(memory_space=pl.ANY)


def params(mib):
    return pltpu.CompilerParams(vmem_limit_bytes=mib * 1024 * 1024)


def in_hbm(value):
    return pltpu.with_memory_space_constraint(value, pltpu.HBM)


def swapped(value, first, second):
    half = value.shape[1] // 2
    lane = lax.broadcasted_iota(jnp.int32, value.shape, 1)
    sign = jnp.where(lane < half, first, second).astype(jnp.float32)
    return pltpu.roll(value.astype(jnp.float32), half, 1) * sign


def turn_and_sum(lefts, table_ref, first, phased_ref, sum_ref, at_block=lambda r: r):
    slots, colours, _, tiles, _, width = phased_ref.shape
    half = width // 2
    spaces, _, count, rows, _ = sum_ref.shape
    for s in range(slots):
        totals = [None] * (count // 2)
        for c in range(colours):
            left = [lefts(s, c, t) for t in range(tiles)]
            for t in range(tiles):
                at = slice(t * width, (t + 1) * width)
                real = left[t][:half].astype(jnp.float32)
                imag = left[t][half:].astype(jnp.float32)
                for m in range(count):
                    row = slice(first + m, first + m + 1)
                    cosine = jnp.broadcast_to(table_ref[0, row, at], (half, width))
                    sine = jnp.broadcast_to(table_ref[1, row, at], (half, width))
                    top = m % 2 * width
                    phased_ref[s, c, m // 2, t, top : top + half] = (
                        cosine * real - sine * imag
                    ).astype(jnp.bfloat16)
                    phased_ref[s, c, m // 2, t, top + half : top + width] = (
                        sine * real + cosine * imag
                    ).astype(jnp.bfloat16)
            left = jnp.concatenate(left, axis=1)
            for p in range(count // 2):
                right = jnp.concatenate([phased_ref[s, c, p, t] for t in range(tiles)], axis=1)
                product = lax.dot_general(
                    left, right, (((1,), (1,)), ((), ())), preferred_element_type=jnp.float32
                )
                totals[p] = product if totals[p] is None else totals[p] + product
        for m in range(count):
            block = totals[m // 2][:, m % 2 * width : (m % 2 + 1) * width]
            value = block[:half] + swapped(block[half:], 1.0, -1.0)
            for r in range(spaces):
                sum_ref[at_block(r), s, m] = value[r * rows : (r + 1) * rows]


def given_kernel(place_hbm, mom_hbm, x_hbm, out_ref, table_ref, turned_ref, *scratch):
    x_ref, place_ref, mom_ref, phased_ref, sems = scratch
    _, _, sites, width = x_ref.shape
    spaces, _, count, _, _ = out_ref.shape
    moms = mom_ref.shape[1]
    spins = moms // count
    x_copy = pltpu.make_async_copy(x_hbm, x_ref, sems.at[0])
    mom_copy = pltpu.make_async_copy(mom_hbm, mom_ref, sems.at[1])
    place_copy = pltpu.make_async_copy(place_hbm, place_ref, sems.at[2])
    mom_copy.start()
    place_copy.start()
    x_copy.start()
    row = lax.broadcasted_iota(jnp.int32, (moms, sites), 0)
    site = lax.broadcasted_iota(jnp.int32, (moms, sites), 1)
    place_copy.wait()
    space = place_ref[0]
    spin = place_ref[1]
    site = site + (space * spins + spin) * sites
    coords = (site % LAT, site // LAT % LAT, site // (LAT * LAT))
    mom_copy.wait()
    wave = jnp.zeros((moms, sites), jnp.int32)
    for d in range(3):
        value = jnp.zeros((moms, sites), jnp.int32)
        for m in range(moms):
            value = jnp.where(
                row == m, mom_ref[d, lax.rem(spin + m // count, spins) * count + m % count], value
            )
        wave = wave + value * coords[d]
    angle = (wave & (LAT - 1)).astype(jnp.float32) * (TURN / LAT)
    table_ref[0] = jnp.cos(angle)
    table_ref[1] = jnp.sin(angle)
    x_copy.wait()

    def lefts(s, c, t):
        value = x_ref[s, c, t * width : (t + 1) * width].T
        turned_ref[s, c, t] = value
        return value

    turn_and_sum(
        lefts, table_ref, count, phased_ref, out_ref, lambda r: lax.rem(r + spaces - space, spaces)
    )


def given(place, mom_t, x, spaces, spins):
    slots, colours, sites, width = x.shape
    moms = mom_t.shape[1]
    count = moms // spins
    shape = (spaces, slots, count, width // 2 // spaces, width)
    tiles = sites // width
    return pl.pallas_call(
        given_kernel,
        out_shape=[
            jax.ShapeDtypeStruct(shape, jnp.float32),
            jax.ShapeDtypeStruct((2, moms, sites), jnp.float32),
            jax.ShapeDtypeStruct((slots, colours, tiles, width, width), x.dtype),
        ],
        in_specs=[ANY, ANY, ANY],
        out_specs=[VMEM] * 3,
        scratch_shapes=[
            pltpu.VMEM(x.shape, x.dtype),
            pltpu.SMEM(place.shape, jnp.int32),
            pltpu.SMEM(mom_t.shape, jnp.int32),
            pltpu.VMEM((slots, colours, count // 2, tiles, 2 * width, width), jnp.bfloat16),
            pltpu.SemaphoreType.DMA((3,)),
        ],
        compiler_params=params(20),
        name="given",
    )(place, in_hbm(mom_t), in_hbm(x))


def kept_kernel(place_hbm, table_ref, turned_ref, out_ref, place_ref, phased_ref, sum_ref, sem):
    spaces = out_ref.shape[0]
    place_copy = pltpu.make_async_copy(place_hbm, place_ref, sem)
    place_copy.start()
    turn_and_sum(lambda s, c, t: turned_ref[s, c, t], table_ref, 0, phased_ref, sum_ref)
    place_copy.wait()
    for j in range(spaces):
        out_ref[j] = sum_ref[lax.rem(place_ref[0] + j, spaces)]


def kept(place, table, turned, spaces, spins):
    slots, colours, tiles, width, _ = turned.shape
    count = table.shape[1] // spins
    shape = (spaces, slots, count, width // 2 // spaces, width)
    return pl.pallas_call(
        kept_kernel,
        out_shape=jax.ShapeDtypeStruct(shape, jnp.float32),
        in_specs=[ANY, VMEM, VMEM],
        out_specs=VMEM,
        scratch_shapes=[
            pltpu.SMEM(place.shape, jnp.int32),
            pltpu.VMEM((slots, colours, count // 2, tiles, 2 * width, width), jnp.bfloat16),
            pltpu.VMEM(shape, jnp.float32),
            pltpu.SemaphoreType.DMA,
        ],
        compiler_params=params(20),
        name="kept",
    )(place, table, turned)


def doubled_kernel(tau_ref, out_ref):
    pairs, vectors, wide = tau_ref.shape
    width = 2 * vectors
    for k in range(pairs):
        out_ref[k, :vectors] = tau_ref[k]
        for g in range(wide // width):
            at = slice(g * width, (g + 1) * width)
            out_ref[k, vectors:, at] = swapped(tau_ref[k, :, at], -1.0, 1.0).astype(jnp.bfloat16)


def doubled(perambulators):
    pairs, vectors, wide = perambulators.shape
    return pl.pallas_call(
        doubled_kernel,
        out_shape=jax.ShapeDtypeStruct((pairs, 2 * vectors, wide), perambulators.dtype),
        in_specs=[VMEM],
        out_specs=VMEM,
        compiler_params=params(8),
        name="doubled",
    )(perambulators)


def halfway_kernel(right_ref, *rest):
    sinks, out_ref, turn_ref = rest[:-2], rest[-2], rest[-1]
    pairs, count, rows, width = sinks[0].shape
    lines = len(sinks) * count * rows

    def step(k, carry):
        left = jnp.concatenate([sink[k].reshape(count * rows, width) for sink in sinks], axis=0)
        product = jnp.dot(left, right_ref[k], preferred_element_type=jnp.float32)
        for g in range(SPINS):
            turn_ref[pl.ds(g, lines, stride=SPINS + 1), :] = product[
                :, g * width : (g + 1) * width
            ]
        for n in range(lines):
            out_ref[k, n * SPINS : (n + 1) * SPINS] = turn_ref[
                n * (SPINS + 1) : n * (SPINS + 1) + SPINS
            ].astype(jnp.bfloat16)
        return carry

    lax.fori_loop(0, pairs, step, 0)


def halfway(right, sinks):
    pairs, count, rows, width = sinks[0].shape
    lines = len(sinks) * count * rows * SPINS
    return pl.pallas_call(
        halfway_kernel,
        out_shape=jax.ShapeDtypeStruct((pairs, lines, width), jnp.bfloat16),
        in_specs=[VMEM] * (1 + len(sinks)),
        out_specs=VMEM,
        scratch_shapes=[pltpu.VMEM((lines // SPINS * (SPINS + 1) + SPINS, width), jnp.float32)],
        compiler_params=params(8),
        name="halfway",
    )(right, *sinks)


def loops_kernel(place_ref, half_ref, *rest, spaces, spins, back):
    sources = rest[:spaces]
    out_hbm, stage_ref, sem = rest[-3:]
    pairs, part, rows, spinors, width = stage_ref.shape
    block = sources[0].shape[2]
    count = rows * spinors
    where = jnp.broadcast_to(place_ref[:1, :], (block, width))
    here = [where == space for space in range(spaces)]
    owner = lax.rem(place_ref[1, 0] + spins - back, spins)
    zeros = jnp.zeros((width, width), jnp.bfloat16)
    for k in range(pairs):
        for m in range(0, part, 2):
            rights = []
            for i in range(2):
                blocks = [source[k, m + i].astype(jnp.float32) for source in sources]
                ordered = []
                for r in range(spaces):
                    value = blocks[0]
                    for j in range(1, spaces):
                        value = jnp.where(here[(r + j) % spaces], blocks[j], value)
                    ordered.append(value)
                source = jnp.concatenate(ordered, axis=0)
                turned = swapped(source, -1.0, 1.0)
                rights.append(jnp.concatenate([source, turned], axis=0).astype(jnp.bfloat16))
            right = jnp.concatenate(
                [
                    jnp.concatenate([rights[0], zeros], axis=1),
                    jnp.concatenate([zeros, rights[1]], axis=1),
                ],
                axis=0,
            )
            first = (back * part + m) * count
            left = jnp.concatenate(
                [half_ref[k, first + i * count : first + (i + 1) * count] for i in range(2)], axis=1
            )
            product = lax.dot_general(
                left, right, (((1,), (1,)), ((), ())), preferred_element_type=jnp.float32
            ).astype(jnp.bfloat16)
            for i in range(2):
                stage_ref[k, m + i] = product[:, i * width : (i + 1) * width].reshape(
                    rows, spinors, width
                )
            pltpu.make_async_copy(
                stage_ref.at[k, pl.ds(m, 2)], out_hbm.at[k, pl.ds(owner * part + m, 2)], sem
            ).start()
    pltpu.make_async_copy(stage_ref, out_hbm.at[:, pl.ds(owner * part, part)], sem).wait()


def loops(place_rows, half, sources, back, spins, before):
    pairs, lines, width = half.shape
    spaces = len(sources)
    _, part, _, _ = sources[0].shape
    rows = lines // (spins * part * SPINS)
    operands = [place_rows, half, *sources] + ([] if before is None else [before])
    return pl.pallas_call(
        functools.partial(loops_kernel, spaces=spaces, spins=spins, back=back),
        out_shape=jax.ShapeDtypeStruct((pairs, spins * part, rows, SPINS, width), jnp.bfloat16),
        in_specs=[VMEM] * (2 + spaces) + ([] if before is None else [HBM]),
        out_specs=HBM,
        scratch_shapes=[
            pltpu.VMEM((pairs, part, rows, SPINS, width), jnp.bfloat16),
            pltpu.SemaphoreType.DMA,
        ],
        input_output_aliases={} if before is None else {2 + spaces: 0},
        compiler_params=params(16),
    )(*operands)


def shifted(value, axis, by):
    size = lax.axis_size(axis)
    return lax.ppermute(value, axis, [(i, (i + by) % size) for i in range(size)])


def around(value, axis):
    parts = [value]
    for j in range(1, lax.axis_size(axis)):
        parts.append(shifted(value, axis, j))
    return parts


def targets(size):
    ring = [0, *range(1, size, 2), *reversed(range(2, size, 2))]
    place = {member: n for n, member in enumerate(ring)}
    return [[ring[(place[i] + j) % size] for i in range(size)] for j in range(1, size)]


def exchanged(value, axis):
    parts = [value]
    for to in targets(lax.axis_size(axis)):
        parts.append(lax.ppermute(value, axis, list(enumerate(to))))
    return parts


def arrivals(size):
    table = [[0] * size for _ in range(size)]
    for n, to in enumerate(targets(size)):
        for sender, receiver in enumerate(to):
            table[receiver][sender] = n + 1
    return table


def selected(index, candidates):
    flag = index[:, None, None, None]
    result = jnp.broadcast_to(candidates[0], (index.shape[0],) + candidates[0].shape)
    for n in range(1, len(candidates)):
        result = jnp.where(flag == n, candidates[n], result)
    return result


def per_device(eigenvectors, momenta, time_pairs, slot_map, perambulators):
    spaces = lax.axis_size("space")
    spins = lax.axis_size("spin")
    slots = eigenvectors.shape[0]
    place = jnp.stack([lax.axis_index("space"), lax.axis_index("spin")]).astype(jnp.int32)
    place_rows = jnp.broadcast_to(place[:, None], (2, 2 * perambulators.shape[1]))
    times = slot_map.shape[0]
    named = time_pairs[:, :, None] == lax.iota(jnp.int32, times)
    slot = jnp.sum(jnp.where(named, slot_map, 0), axis=-1)
    members = lax.axis_size("tm")
    table = jnp.array(arrivals(members), jnp.int32)
    row = jnp.sum(
        jnp.where((lax.iota(jnp.int32, members) == lax.axis_index("tm"))[:, None], table, 0), 0
    )
    held = (slot // slots)[..., None] == lax.iota(jnp.int32, members)
    index = jnp.sum(jnp.where(held, row, 0), axis=-1) * slots + slot % slots

    spin = lax.axis_index("spin")
    x = jnp.transpose(eigenvectors, (0, 2, 1, 3))
    send, table, turned = given(place, momenta.T, x, spaces, spins)
    received = shifted(send, "spin", 1)
    total = kept(place, table, turned, spaces, spins)
    total = total + received
    row_share = total[0]
    for j in range(1, spaces):
        value = shifted(total[j].astype(jnp.bfloat16), "space", j)
        row_share = row_share + value.astype(jnp.float32)
    row_share = row_share.astype(jnp.bfloat16)
    arrived = exchanged(row_share, "tm")
    candidates = [value[s] for value in arrived for s in range(slots)]
    early = len(candidates) - slots
    chosen = [selected(index[:, side], candidates[:early]) for side in range(2)]
    chosen = lax.optimization_barrier(chosen)
    for n in range(early, len(candidates)):
        chosen = [
            jnp.where(index[:, side, None, None, None] == n, candidates[n], chosen[side])
            for side in range(2)
        ]
    sink_share, source_share = chosen
    rows = sink_share.shape[2] // spins
    sinks = []
    for i in range(spins):
        block = lax.dynamic_slice_in_dim(sink_share, (spin + i) % spins * rows, rows, axis=2)
        if i:
            block = shifted(block, "spin", i)
        sinks.append(block)
    right = doubled(perambulators)
    half = halfway(right, sinks)
    far = around(source_share, "space")
    near = [around(value, "spin") for value in far]
    result = None
    for back in range(spins):
        sources = [group[back] for group in near]
        result = loops(place_rows, half, sources, back, spins, result)
    return result


def solution(mesh):
    placed = (
        P(("cfg", "tm"), ("space", "spin"), None, None),
        P(),
        P(("cfg", "tm"), None),
        P(),
        P(("cfg", "tm"), None, None),
    )

    return jax.shard_map(
        per_device,
        mesh=mesh,
        in_specs=placed,
        out_specs=P(("cfg", "tm"), None, ("space", "spin"), None, None),
        check_vma=False,
    )
```
